512 devices in a mesh: dp: 8 (over y), expert: 64 (over z, x, core).
Axes of the slice: x: 4, y: 8, z: 8, core: 2. Of those that a mesh axis runs over, the one named last changes fastest.
Arguments:
- tokens: bfloat16 [4096, 2880], P(('dp', 'expert')), may hold values from -6 to 6
- routes: int32 [2, 4096, 4], P(None, ('dp', 'expert')), may hold values from 0 to 63, all different within a row; in each aligned block of 8 rows (0 to 7, 8 to 15, ..., all dimensions but the last counted through in order) at most 1 rows name the same one
- placement: int32 [2, 64], replicated, may hold values from 0 to 63, each once within a row
- up_weight: bfloat16 [2, 64, 2880, 1440], P(None, 'expert', None, 'dp'), may hold values from -0.109375 to 0.109375
- down_weight: bfloat16 [2, 64, 1440, 2880], P(None, 'expert', 'dp'), may hold values from -0.15625 to 0.15625
- router_weight: bfloat16 [2, 64, 2880], P(None, 'expert'), may hold values from -0.21875 to 0.21875
Outputs:
- final_stream: bfloat16 [4096, 2880], P(('dp', 'expert'))
The draws below stay inside these ranges and needn't reach their ends.
Inputs may be any that keep to these rules, and one draw needn't show every extreme that they name: `routes`: each row names 4 different experts. Within one layer's rows of one device no expert is named by more than 1 row, and some device names some expert exactly 1 times. `placement`: each layer's row is a permutation of the slots.
All inputs are finite; a program needn't handle non-finite values.
Results may differ from the reference program's by a relative error of at most 0.008.
Values may be sent and summed in bfloat16 or wider, within the bound.
A program may use at most 64 MiB of HBM per device.

```python
import math
import jax
import jax.numpy as jnp
import numpy as np
from jax import lax

D = 2880
TOPK = 4
FF = 1440
LAYERS = 2
TOK_DEV = 8
EXPERTS = 64
FF_DEV = 180
CAP = 1
TOKENS = 4096
N_DP = 8
N_EXPERT = 64


def levels(stream_key, extent, split, least, largest):
    factor_of, own = 1.0, jax.random.fold_in(stream_key, 6)
    for position, parts in split:
        heights = jnp.exp(jax.random.uniform(jax.random.fold_in(own, position), (parts,), jnp.float32, least / len(split), largest / len(split)))
        factor_of = factor_of * jnp.repeat(heights, extent[position] // parts).reshape([-1 if axis == position else 1 for axis in range(len(extent))])
    return factor_of


def assign_block(own_key, own, number, rows, count, top, reach, slope):
    ranking = jax.random.permutation(own_key, count)
    crowded, usual = load_shares(count, rows * top, reach, slope, True), load_shares(count, rows * top, reach, slope, False)
    places = jnp.arange(count)

    def named(sizes, rotation):
        used = int((sizes > 0).sum())
        fixed = max(1, used // 4)
        moved = fixed + (places - fixed + rotation * (used - fixed)) % max(1, count - fixed)
        return jnp.zeros((count,), jnp.int32).at[ranking[jnp.where(places < fixed, places, moved)]].set(jnp.asarray(sizes, jnp.int32))

    sizes = jnp.where(number % 4 == 0, named(crowded, number // 4), named(usual, number - number // 4 - 1))
    mixed = jax.random.permutation(jax.random.fold_in(own, 3), count)
    giver, receiver = mixed[0:count // 2 * 2:2], mixed[1:count // 2 * 2:2]
    room = jnp.minimum(sizes[giver] - 1, reach - sizes[receiver]) // 2
    room = jnp.where((giver == ranking[0]) | (receiver == ranking[0]) | (sizes[receiver] == 0), 0, jnp.maximum(room, 0))
    moved = jax.random.randint(jax.random.fold_in(own, 4), (count // 2,), 0, 1 << 20) % (room + 1)
    sizes = sizes.at[giver].add(-moved).at[receiver].add(moved)
    items = jnp.searchsorted(jnp.cumsum(sizes), jnp.arange(rows * top), side="right").astype(jnp.int32)
    listing = items.reshape(top, rows).T
    listing = listing[jax.random.permutation(jax.random.fold_in(own, 1), rows)]
    rotation = jax.random.randint(jax.random.fold_in(own, 2), (rows, 1), 0, top)
    return jnp.take_along_axis(listing, (jnp.arange(top)[None, :] + rotation) % top, axis=1)


def load_shares(count, total, reach, slope, full):
    portions = [(1 << 20) // math.isqrt(rank ** slope) + 1 for rank in range(1, count + 1)]
    largest = reach if full else min(reach, max(-(-total // count), total * portions[0] // sum(portions)))
    least = 1 if total - largest >= count - 1 else 0
    holding, spare = [largest] + [least] * (count - 1), total - largest - least * (count - 1)
    while spare > 0:
        movable = [i for i in range(1, count) if holding[i] < largest] or [i for i in range(1, count) if holding[i] < reach]
        whole, budget = sum([portions[i] for i in movable]), spare
        for i in movable:
            extra = min(reach - holding[i], max(1, budget * portions[i] // whole), spare)
            holding[i] = holding[i] + extra
            spare = spare - extra
    return np.array(holding)


def bell_draw(key, extent, width, most, split=(), kind=jnp.bfloat16):
    entries = width * jax.random.normal(key, extent, jnp.float32)
    if split:
        entries = entries * levels(key, extent, split, -0.22, 0.18)
    return jnp.clip(entries, -most, most).astype(kind)


def setup_inputs(seed: int = 0) -> dict:
    splits = jax.random.split(jax.random.key(seed), 7)
    tokens = bell_draw(splits[0], (TOKENS, D), 1.0, 6.0, ((0, 512),))
    routes_keys = jax.random.split(jax.random.fold_in(splits[1], 1), LAYERS * TOKENS // TOK_DEV)
    routes_turns = jax.random.permutation(jax.random.fold_in(splits[1], 3), LAYERS * TOKENS // TOK_DEV)
    routes = jax.vmap(lambda own, number: assign_block(jax.random.fold_in(splits[1], 2), own, number, TOK_DEV, EXPERTS, TOPK, CAP, 1))(routes_keys, routes_turns).reshape((LAYERS, TOKENS, TOPK))
    placement = jax.vmap(lambda own: jax.random.permutation(own, EXPERTS))(jax.random.split(splits[2], LAYERS)).reshape((LAYERS, EXPERTS)).astype(jnp.int32)
    up_weight = bell_draw(splits[3], (LAYERS, EXPERTS, D, FF), D ** -0.5, 0.109375, ((1, 64), (3, 8)))
    down_weight = bell_draw(splits[4], (LAYERS, EXPERTS, FF, D), FF ** -0.5, 0.15625, ((1, 64), (2, 8)))
    router_weight = bell_draw(splits[5], (LAYERS, EXPERTS, D), (D // 4) ** -0.5, 0.21875, ((1, 64),))
    return dict(tokens=tokens, routes=routes, placement=placement, up_weight=up_weight, down_weight=down_weight, router_weight=router_weight)


def rms_rows(stream):
    values = stream.astype(jnp.float32)
    inverse = lax.rsqrt(lax.optimization_barrier(jnp.mean(values * values, axis=-1, keepdims=True)) + 1e-05)
    return (values * inverse).astype(jnp.bfloat16)

def layer_step(stream, packed):
    route_rows, place_row, up_layer, down_layer, router_layer = packed
    normed = rms_rows(stream)
    target = place_row[route_rows].reshape(-1).astype(jnp.int32)
    row_order = jnp.argsort(target, stable=True).astype(jnp.int32)
    sorted_target = target[row_order]
    slot_ids = jnp.arange(EXPERTS, dtype=jnp.int32)
    counts = lax.optimization_barrier(jnp.sum((target[:, None] == slot_ids[None, :]).astype(jnp.int32), axis=0))
    starts = (jnp.cumsum(counts) - counts).astype(jnp.int32)
    slot_rows = N_DP * N_EXPERT * CAP
    picked = jnp.concatenate([normed[row_order // TOPK], jnp.zeros((slot_rows, D), jnp.bfloat16)], axis=0)

    def per_slot(slot_index):
        slot_in = lax.dynamic_slice_in_dim(picked, starts[slot_index], slot_rows, 0)
        hidden = jax.nn.silu(jnp.dot(slot_in, up_layer[slot_index], preferred_element_type=jnp.float32)).astype(jnp.bfloat16)
        blocks = hidden.astype(jnp.float32).reshape(slot_rows, N_DP, FF_DEV)
        down_blocks = down_layer[slot_index].astype(jnp.float32).reshape(N_DP, FF_DEV, D)
        part_sums = jnp.einsum('rbf,bfd->rbd', blocks, down_blocks).astype(jnp.bfloat16)
        output = lax.optimization_barrier(jnp.sum(part_sums.astype(jnp.float32), axis=1))
        affinity = jax.nn.sigmoid(jnp.dot(slot_in, router_layer[slot_index], preferred_element_type=jnp.float32)).astype(jnp.bfloat16)
        return (output, affinity)
    outputs, affinity = lax.map(per_slot, slot_ids)
    within = jnp.arange(target.shape[0], dtype=jnp.int32) - starts[sorted_target]
    sorted_out = outputs[sorted_target, within]
    sorted_gate = affinity[sorted_target, within]
    row_out = jnp.zeros_like(sorted_out).at[row_order].set(sorted_out).reshape(-1, TOPK, D)
    row_gate = jnp.zeros_like(sorted_gate).at[row_order].set(sorted_gate).reshape(-1, TOPK).astype(jnp.float32)
    numerator = lax.optimization_barrier(jnp.sum(row_gate[:, :, None] * row_out, axis=1))
    denominator = jnp.maximum(lax.optimization_barrier(jnp.sum(row_gate, axis=1)), 0.5)
    updated = stream.astype(jnp.float32) + numerator / denominator[:, None]
    return (updated.astype(jnp.bfloat16), None)

def reference(tokens, routes, placement, up_weight, down_weight, router_weight):
    result_stream, unused = lax.scan(layer_step, tokens, (routes, placement, up_weight, down_weight, router_weight))
    return result_stream
```

```python
import functools

import jax
import jax.numpy as jnp
from jax import lax
from jax.experimental import pallas as pl
from jax.experimental.pallas import tpu as pltpu
from jax.sharding import PartitionSpec as P

MESH = pl.DeviceIdType.MESH
F32, BF16 = jnp.float32, jnp.bfloat16
NT = (((1,), (1,)), ((), ()))


def flat(value):
    width = value.shape[-1]
    return value.astype(F32).reshape(-1, width).astype(BF16)


def flat32(value):
    return value.astype(F32).reshape(-1, value.shape[-1])


def hops(direction, half, n):
    return n // 2 if (direction == 1) == (half == 0) else n // 2 - 1


def kernel(
    dims,
    tokens,
    routes,
    placement,
    router,
    up,
    down,
    out,
    stream,
    hot,
    up_v,
    down_v,
    router_v,
    zin1,
    xo1,
    rows1,
    toks2,
    xo2,
    rows2,
    h1,
    h2,
    hid1,
    hid2,
    gate1,
    gate2,
    part1,
    comb2,
    rs1o,
    rs1i,
    xr1o,
    xr1i,
    zr1o,
    zr1i,
    xr2o,
    xr2i,
    rs2o,
    rs2i,
    yr2o,
    yr2i,
    weight_sem,
    send_sem,
    z1_sem,
    x1_sem,
    ring1_sem,
    y2_sem,
    ring2_sem,
    x2_sem,
    rs1_sem,
    xr1_sem,
    zr1_sem,
    xr2_sem,
    rs2_sem,
    yr2_sem,
):
    ny, nz, nj, layers, features, w1, f2, ff = dims
    hj, hy = nj // 2, ny // 2
    y = lax.axis_index("dp")
    e = lax.axis_index("expert")
    z, j = e // nj, e % nj
    lanes = 128

    def at_y(other):
        return (other, e)

    def at_z(other):
        return (y, other * nj + j)

    def at_j(other):
        return (y, z * nj + other)

    def turn(a, n):
        return lax.rem(a + 2 * n, n)

    barrier = pltpu.get_barrier_semaphore()
    for d in range(1, ny):
        pl.semaphore_signal(barrier, inc=1, device_id=at_y(turn(y + d, ny)), device_id_type=MESH)
    for d in range(1, nz):
        pl.semaphore_signal(barrier, inc=1, device_id=at_z(turn(z + d, nz)), device_id_type=MESH)
    for d in range(1, nj):
        pl.semaphore_signal(barrier, inc=1, device_id=at_j(turn(j + d, nj)), device_id_type=MESH)

    weights = []
    for layer in range(layers):
        weights.append(
            (
                pltpu.make_async_copy(up.at[layer, 0], up_v.at[layer], weight_sem.at[layer, 0]),
                pltpu.make_async_copy(down.at[layer, 0], down_v.at[layer], weight_sem.at[layer, 1]),
            )
        )
        for copy in weights[-1]:
            copy.start()

    for layer in range(layers):
        picks = routes[layer]
        count = placement.shape[1]
        names = lax.broadcasted_iota(jnp.int32, (picks.shape[0], count), 1)
        named = jnp.zeros((picks.shape[0], count), F32)
        for k in range(picks.shape[1]):
            named = named + jnp.where(picks[:, k : k + 1] == names, 1.0, 0.0)
        slot_of = jnp.broadcast_to(placement[layer : layer + 1, :], (lanes, count))
        slots = lax.broadcasted_iota(jnp.int32, (lanes, count), 0)
        for which, shift in ((0, 0), (1, lanes // 2)):
            serves = jnp.where(slot_of + shift == slots, 1.0, 0.0).astype(BF16)
            hot[layer, which] = lax.dot_general(
                named.astype(BF16), serves, NT, preferred_element_type=F32
            )
    for layer in range(layers):
        gate_row = jnp.broadcast_to(router[layer].astype(F32), (lanes, features)).astype(BF16)
        router_v[layer, :, 0:features] = gate_row

    stream[...] = jnp.zeros_like(stream)
    stream[:, 0:features] = tokens[...].astype(F32)

    def picker(blocks, low):
        rows = nj * blocks
        tokens_in = blocks * 8
        return rows, tokens_in, low

    def pick_matrix(hots, blocks, low):
        rows, columns, low = picker(blocks, low)
        row = lax.broadcasted_iota(jnp.int32, (rows, lanes), 0)
        slot = lax.broadcasted_iota(jnp.int32, (rows, lanes), 1)
        wanted = jnp.where(slot == low + z * nj + row // blocks, 1.0, 0.0).astype(BF16)
        same = (
            lax.broadcasted_iota(jnp.int32, (rows, columns), 0) % blocks
            == lax.broadcasted_iota(jnp.int32, (rows, columns), 1) // 8
        )
        product = lax.dot_general(wanted, hots, NT, preferred_element_type=F32)
        return jnp.where(same, product, 0.0).astype(BF16)

    def place_matrix(hots, blocks, low):
        rows, columns, low = picker(blocks, low)
        row = lax.broadcasted_iota(jnp.int32, (rows, lanes), 0)
        slot = lax.broadcasted_iota(jnp.int32, (rows, lanes), 1)
        wanted = jnp.where(slot == low + z * nj + row // blocks, 1.0, 0.0).astype(BF16)
        same = (
            lax.broadcasted_iota(jnp.int32, (columns, rows), 1) % blocks
            == lax.broadcasted_iota(jnp.int32, (columns, rows), 0) // 8
        )
        product = lax.dot_general(hots, wanted, NT, preferred_element_type=F32)
        return jnp.where(same, product, 0.0).astype(BF16)

    def send(src, dst, sent, landed, device):
        pltpu.make_async_remote_copy(
            src_ref=src, dst_ref=dst, send_sem=sent, recv_sem=landed, device_id=device, device_id_type=MESH
        ).start()

    def wait_bytes(ref, sem):
        pltpu.make_async_copy(ref, ref, sem).wait()

    (S_Z1, S_X1, S_RING1, S_Y2, S_RING2, S_X2, S_RS1, S_XR1, S_ZR1, S_XR2, S_RS2, S_YR2) = range(12)

    def layer_body(l, carry):
        sent = lambda which: send_sem.at[l, which]

        values = stream[...]
        mean = jnp.sum(values * values, axis=1, keepdims=True) * (1.0 / features)
        normed = values * lax.rsqrt(mean + 1e-05)
        zin1[l, z, :, 0:w1] = normed[:, 0:w1].astype(BF16)
        zin1[l, z, :, w1 : w1 + lanes] = hot[l, 0].astype(BF16)
        width2 = normed.shape[1] - w1
        toks2[l, z, y, :, 0 : width2 - lanes] = normed[:, w1 : w1 + width2 - lanes].astype(BF16)
        toks2[l, z, y, :, width2 - lanes : width2] = (normed[:, w1 + width2 - lanes :] + hot[l, 1]).astype(BF16)

        @pl.when(l == 0)
        def _():
            pl.semaphore_wait(barrier, ny + nz + nj - 3)

        for d in range(1, ny):
            block = toks2.at[l, z, y]
            send(block, block, sent(S_Y2), y2_sem.at[l], at_y(turn(y + d, ny)))
        for d in range(1, nz):
            block = zin1.at[l, z]
            send(block, block, sent(S_Z1), z1_sem.at[l], at_z(turn(z + d, nz)))

        wait_bytes(toks2.at[l, 0, 0 : ny - 1], y2_sem.at[l])

        def ring2_send(origin, direction, half, step):
            part = toks2.at[l, origin, half * hy : (half + 1) * hy]
            send(part, part, sent(S_RING2), ring2_sem.at[l, (direction + 1) // 2, half, step - 1], at_z(turn(z + direction, nz)))

        def ring1_send(origin, direction, half, step):
            part = rows1.at[l, origin, half * hj : (half + 1) * hj]
            send(part, part, sent(S_RING1), ring1_sem.at[l, (direction + 1) // 2, half, step - 1], at_y(turn(y + direction, ny)))

        def ring2_step(step):
            for direction in (1, -1):
                origin = turn(z - direction * step, nz)
                for half in (0, 1):
                    if hops(direction, half, nz) >= step:
                        wait_bytes(
                            toks2.at[l, origin, half * hy : (half + 1) * hy],
                            ring2_sem.at[l, (direction + 1) // 2, half, step - 1],
                        )
                        if hops(direction, half, nz) > step:
                            ring2_send(origin, direction, half, step + 1)

        def ring1_step(step):
            for direction in (1, -1):
                origin = turn(y - direction * step, ny)
                for half in (0, 1):
                    if hops(direction, half, ny) >= step:
                        wait_bytes(
                            rows1.at[l, origin, half * hj : (half + 1) * hj],
                            ring1_sem.at[l, (direction + 1) // 2, half, step - 1],
                        )
                        if hops(direction, half, ny) > step:
                            ring1_send(origin, direction, half, step + 1)

        def exchange2(zc):
            chunk = flat(toks2[l, zc])
            pick = pick_matrix(chunk[:, width2 - lanes :], ny, lanes // 2)
            rows = jnp.dot(pick, chunk[:, 0:f2], preferred_element_type=F32)
            xo2[l, zc] = rows.reshape(nj, ny, f2).astype(BF16)
            rows2[l, zc, j] = xo2[l, zc, j]
            for d in range(1, nj):
                other = turn(j + d, nj)
                send(xo2.at[l, zc, other], rows2.at[l, zc, j], sent(S_X2), x2_sem.at[l, zc], at_j(other))

        def up1(yc):
            rows = flat(rows1[l, yc])
            at = pl.ds(yc * (nj * nz), nj * nz)
            result = jnp.dot(rows, up_v[l, 0:w1, :], preferred_element_type=F32)
            h1[0, at, :] = result[:, 0:lanes]
            h1[1, at, 0 : ff - lanes] = result[:, lanes:ff]
            h1[2, at, :] = lax.dot_general(rows, router_v[l, :, 0:w1], NT, preferred_element_type=F32)

        def up2(zc):
            wait_bytes(rows2.at[l, zc, 0 : nj - 1], x2_sem.at[l, zc])
            rows = flat(rows2[l, zc])
            at = pl.ds(zc * (nj * ny), nj * ny)
            result = jnp.dot(rows, up_v[l, w1 : w1 + f2, :], preferred_element_type=F32)
            h2[0, at, :] = result[:, 0:lanes]
            h2[1, at, 0 : ff - lanes] = result[:, lanes:ff]
            h2[2, at, :] = lax.dot_general(rows, router_v[l, :, w1 : w1 + f2], NT, preferred_element_type=F32)

        for direction in (1, -1):
            for half in (0, 1):
                if hops(direction, half, nz) >= 1:
                    ring2_send(z, direction, half, 1)

        wait_bytes(zin1.at[l, 0 : nz - 1], z1_sem.at[l])
        chunk1 = flat(zin1[l])
        pick = pick_matrix(chunk1[:, w1:], nz, 0)
        picked = jnp.dot(pick, chunk1[:, 0:w1], preferred_element_type=F32)
        xo1[l] = picked.reshape(nj, nz, w1).astype(BF16)
        rows1[l, y, j] = xo1[l, j]
        for d in range(1, nj):
            other = turn(j + d, nj)
            send(xo1.at[l, other], rows1.at[l, y, j], sent(S_X1), x1_sem.at[l], at_j(other))

        exchange2(z)
        wait_bytes(rows1.at[l, y, 0 : nj - 1], x1_sem.at[l])
        for direction in (1, -1):
            for half in (0, 1):
                if hops(direction, half, ny) >= 1:
                    ring1_send(y, direction, half, 1)

        @pl.when(l == 0)
        def _():
            for pair in weights:
                for copy in pair:
                    copy.wait()

        up1(y)
        steps2, steps1 = nz // 2, ny // 2
        done2 = [z]
        for step in range(1, max(steps1, steps2) + 1):
            if step <= steps2:
                ring2_step(step)
                arrived = [turn(z - step, nz)] if 2 * step == nz else [turn(z - step, nz), turn(z + step, nz)]
                for zc in arrived:
                    exchange2(zc)
                for zc in done2:
                    up2(zc)
                done2 = arrived
            if step <= steps1:
                ring1_step(step)
                for yc in [turn(y - step, ny)] if 2 * step == ny else [turn(y - step, ny), turn(y + step, ny)]:
                    up1(yc)
        for zc in done2:
            up2(zc)

        def silu(v):
            return v / (1.0 + jnp.exp(-v))

        def sigmoid(v):
            return 1.0 / (1.0 + jnp.exp(-v))

        def join1(yc, carry):
            base = pl.multiple_of(yc * (nj * nz), nj * nz)
            total = []
            for lane in range(3):
                tiles = [
                    h2[lane, pl.ds(jc * ny + yc, nz, stride=nj * ny), :] for jc in range(nj)
                ]
                total.append(h1[lane, pl.ds(base, nj * nz), :] + jnp.concatenate(tiles, axis=0))
            hid1[yc, :, 0:lanes] = silu(total[0]).astype(BF16)
            hid1[yc, :, lanes:ff] = silu(total[1])[:, 0 : ff - lanes].astype(BF16)
            gate1[yc] = sigmoid(total[2]).astype(BF16).astype(F32)
            return carry

        def join2(zc, carry):
            base = pl.multiple_of(zc * (nj * ny), nj * ny)
            total = []
            for lane in range(3):
                tiles = [
                    h1[lane, pl.ds(jc * nz + zc, ny, stride=nj * nz), :] for jc in range(nj)
                ]
                total.append(h2[lane, pl.ds(base, nj * ny), :] + jnp.concatenate(tiles, axis=0))
            hid2[zc, :, 0:lanes] = silu(total[0]).astype(BF16)
            hid2[zc, :, lanes:ff] = silu(total[1])[:, 0 : ff - lanes].astype(BF16)
            gate2[zc] = sigmoid(total[2]).astype(BF16).astype(F32)
            return carry

        lax.fori_loop(0, nz, join2, 0)
        lax.fori_loop(0, ny, join1, 0)

        def down2(zc):
            result = jnp.dot(hid2[zc], down_v[l, :, w1 : w1 + f2], preferred_element_type=F32)
            result = result * gate2[zc][:, 0:1]
            xr2o[l, zc] = result.reshape(nj, ny, f2).astype(BF16)
            xr2i[l, zc, j] = xr2o[l, zc, j]
            for d in range(1, nj):
                other = turn(j + d, nj)
                send(xr2o.at[l, zc, other], xr2i.at[l, zc, j], sent(S_XR2), xr2_sem.at[l, zc], at_j(other))

        def down1(yc):
            result = jnp.dot(hid1[yc], down_v[l, :, 0:w1], preferred_element_type=F32)
            result = result * gate1[yc][:, 0:1]
            part1[yc] = result.reshape(nj, nz, w1).astype(BF16)

        def combine2(zc):
            wait_bytes(xr2i.at[l, zc, 0 : nj - 1], xr2_sem.at[l, zc])
            place = place_matrix(flat(toks2[l, zc, :, :, width2 - lanes :]), ny, lanes // 2)
            total = jnp.dot(place, flat(xr2i[l, zc]), preferred_element_type=F32)
            comb2[zc] = total.reshape(ny, 8, f2).astype(BF16)

        def slot_of_send(moving, half, step, n):
            long, short = n // 2, n // 2 - 1
            order = []
            for m in (1, -1):
                for h in (0, 1):
                    for s in range(1, hops(-m, h, n) + 1):
                        order.append((m, h, s))
            return order.index((moving, half, step))

        def reduce_step(me, n, size, own, outgoing, incoming, sems, sent_sem, to, step):
            for moving in (1, -1):
                for half in (0, 1):
                    length = hops(-moving, half, n)
                    if length < step:
                        continue
                    dest = turn(me + moving * (length + 1 - step), n)
                    value = own[dest, half * size : (half + 1) * size]
                    slot = slot_of_send(moving, half, step, n)
                    if step > 1:
                        before = slot_of_send(moving, half, step - 1, n)
                        wait_bytes(incoming.at[l, before], sems.at[l, before])
                        value = (value.astype(F32) + incoming[l, before].astype(F32)).astype(BF16)
                    outgoing[l, slot] = value
                    send(outgoing.at[l, slot], incoming.at[l, slot], sent_sem, sems.at[l, slot], to(turn(me + moving, n)))

        def reduce_end(me, n, size, own, incoming, sems):
            halves = []
            for half in (0, 1):
                total = own[me, half * size : (half + 1) * size].astype(F32)
                for moving in (1, -1):
                    length = hops(-moving, half, n)
                    if length >= 1:
                        slot = slot_of_send(moving, half, length, n)
                        wait_bytes(incoming.at[l, slot], sems.at[l, slot])
                        total = total + incoming[l, slot].astype(F32)
                halves.append(total)
            return halves

        def by_distance(me, n):
            order = [turn(me + n // 2, n)]
            for d in range(n // 2 - 1, 0, -1):
                order += [turn(me + d, n), turn(me - d, n)]
            return order + [me]

        order2, order1 = by_distance(z, nz), by_distance(y, ny)
        first2, first1 = min(3, nz), min(3, ny)
        for zc in order2[:first2]:
            down2(zc)
        for yc in order1[:first1]:
            down1(yc)
        reduce_step(y, ny, hj, part1, rs1o, rs1i, rs1_sem, sent(S_RS1), at_y, 1)
        for zc in order2[first2:]:
            down2(zc)
        for yc in order1[first1:]:
            down1(yc)
        for zc in order2[:first2]:
            combine2(zc)
        reduce_step(z, nz, hy, comb2, rs2o, rs2i, rs2_sem, sent(S_RS2), at_z, 1)
        for step in range(2, max(steps1, steps2) + 1):
            for zc in order2[2 * step - 1 : 2 * step + 1]:
                combine2(zc)
            if step <= steps1:
                reduce_step(y, ny, hj, part1, rs1o, rs1i, rs1_sem, sent(S_RS1), at_y, step)
            if step <= steps2:
                reduce_step(z, nz, hy, comb2, rs2o, rs2i, rs2_sem, sent(S_RS2), at_z, step)

        for half, total in enumerate(reduce_end(y, ny, hj, part1, rs1i, rs1_sem)):
            xr1o[l, half * hj : (half + 1) * hj, :, 0:w1] = total.astype(BF16)
        xr1o[l, :, :, w1 : w1 + lanes] = gate1[y].reshape(nj, nz, lanes).astype(BF16)
        xr1i[l, j] = xr1o[l, j]
        for d in range(1, nj):
            other = turn(j + d, nj)
            send(xr1o.at[l, other], xr1i.at[l, j], sent(S_XR1), xr1_sem.at[l], at_j(other))

        for half, total in enumerate(reduce_end(z, nz, hy, comb2, rs2i, rs2_sem)):
            yr2o[l, half * hy : (half + 1) * hy] = total.astype(BF16)
        yr2i[l, y] = yr2o[l, y]
        for d in range(1, ny):
            other = turn(y + d, ny)
            send(yr2o.at[l, other], yr2i.at[l, y], sent(S_YR2), yr2_sem.at[l], at_y(other))

        wait_bytes(xr1i.at[l, 0 : nj - 1], xr1_sem.at[l])
        place1 = place_matrix(flat(zin1[l, :, :, w1 : w1 + lanes]), nz, 0)
        sums = jnp.dot(place1, flat(xr1i[l]), preferred_element_type=F32)
        zr1o[l, :, :, 0:w1] = sums[:, 0:w1].reshape(nz, 8, w1).astype(BF16)
        gates = sums[:, w1:]
        high = gates.astype(BF16).astype(F32)
        lane = lax.broadcasted_iota(jnp.int32, gates.shape, 1)
        pair = jnp.where(lane < lanes // 2, high, gates - high)
        zr1o[l, :, :, w1 : w1 + lanes] = pair.reshape(nz, 8, lanes).astype(BF16)
        zr1i[l, z] = zr1o[l, z]
        for d in range(1, nz):
            other = turn(z + d, nz)
            send(zr1o.at[l, other], zr1i.at[l, z], sent(S_ZR1), zr1_sem.at[l], at_z(other))

        wait_bytes(yr2i.at[l, 0 : ny - 1], yr2_sem.at[l])
        numer2 = jnp.sum(yr2i[l].astype(F32), axis=0)
        wait_bytes(zr1i.at[l, 0 : nz - 1], zr1_sem.at[l])
        both = jnp.sum(zr1i[l].astype(F32), axis=0)
        denom = both[:, w1 : w1 + 1] + both[:, w1 + lanes // 2 : w1 + lanes // 2 + 1]
        denom = jnp.maximum(denom, 0.5)
        stream[:, 0:w1] = (stream[:, 0:w1] + both[:, 0:w1] / denom).astype(BF16).astype(F32)
        stream[:, w1 : w1 + f2] = (stream[:, w1 : w1 + f2] + numer2 / denom).astype(BF16).astype(F32)

        wait_bytes(zin1.at[l, 0 : nz - 1], sent(S_Z1))
        wait_bytes(xo1.at[l, 0 : nj - 1], sent(S_X1))
        wait_bytes(rows1.at[l, 0 : ny - 1], sent(S_RING1))
        wait_bytes(toks2.at[l, 0, 0 : ny - 1], sent(S_Y2))
        wait_bytes(toks2.at[l, 0 : nz - 1], sent(S_RING2))
        wait_bytes(xo2.at[l, :, 0 : nj - 1], sent(S_X2))
        wait_bytes(rs1o.at[l], sent(S_RS1))
        wait_bytes(xr1o.at[l, 0 : nj - 1], sent(S_XR1))
        wait_bytes(zr1o.at[l, 0 : nz - 1], sent(S_ZR1))
        wait_bytes(xr2o.at[l, :, 0 : nj - 1], sent(S_XR2))
        wait_bytes(rs2o.at[l], sent(S_RS2))
        wait_bytes(yr2o.at[l, 0 : ny - 1], sent(S_YR2))
        return carry

    lax.fori_loop(0, layers, layer_body, 0)
    out[...] = stream[:, 0:features].astype(BF16)


def per_device(plane, tokens, routes, placement, up_weight, down_weight, router_weight):
    ny = lax.axis_size("dp")
    nj = plane
    nz = lax.axis_size("expert") // nj
    layers, _, features, ff = up_weight.shape
    w1 = features // 256 * 128
    f2 = features - w1
    padded = -(-features // 128) * 128
    width2 = padded - w1
    hj, hy = nj // 2, ny // 2
    dims = (ny, nz, nj, layers, features, w1, f2, ff)
    rows = ny * nz * nj
    dma = pltpu.SemaphoreType.DMA
    scratch = [
        pltpu.VMEM((8, padded), F32),
        pltpu.VMEM((layers, 2, 8, 128), F32),
        pltpu.VMEM((layers, features, ff), BF16),
        pltpu.VMEM((layers, ff, features), BF16),
        pltpu.VMEM((layers, 128, features), BF16),
        pltpu.VMEM((layers, nz, 8, w1 + 128), BF16),
        pltpu.VMEM((layers, nj, nz, w1), BF16),
        pltpu.VMEM((layers, ny, nj, nz, w1), BF16),
        pltpu.VMEM((layers, nz, ny, 8, width2), BF16),
        pltpu.VMEM((layers, nz, nj, ny, f2), BF16),
        pltpu.VMEM((layers, nz, nj, ny, f2), BF16),
        pltpu.VMEM((3, rows, 128), F32),
        pltpu.VMEM((3, rows, 128), F32),
        pltpu.VMEM((ny, nj * nz, ff), BF16),
        pltpu.VMEM((nz, nj * ny, ff), BF16),
        pltpu.VMEM((ny, nj * nz, 128), F32),
        pltpu.VMEM((nz, nj * ny, 128), F32),
        pltpu.VMEM((ny, nj, nz, w1), BF16),
        pltpu.VMEM((nz, ny, 8, f2), BF16),
        pltpu.VMEM((layers, 2 * (ny - 1), hj, nz, w1), BF16),
        pltpu.VMEM((layers, 2 * (ny - 1), hj, nz, w1), BF16),
        pltpu.VMEM((layers, nj, nz, w1 + 128), BF16),
        pltpu.VMEM((layers, nj, nz, w1 + 128), BF16),
        pltpu.VMEM((layers, nz, 8, w1 + 128), BF16),
        pltpu.VMEM((layers, nz, 8, w1 + 128), BF16),
        pltpu.VMEM((layers, nz, nj, ny, f2), BF16),
        pltpu.VMEM((layers, nz, nj, ny, f2), BF16),
        pltpu.VMEM((layers, 2 * (nz - 1), hy, 8, f2), BF16),
        pltpu.VMEM((layers, 2 * (nz - 1), hy, 8, f2), BF16),
        pltpu.VMEM((layers, ny, 8, f2), BF16),
        pltpu.VMEM((layers, ny, 8, f2), BF16),
        dma((layers, 2)),
        dma((layers, 12)),
        dma((layers,)),
        dma((layers,)),
        dma((layers, 2, 2, ny // 2)),
        dma((layers,)),
        dma((layers, 2, 2, nz // 2)),
        dma((layers, nz)),
        dma((layers, 2 * (ny - 1))),
        dma((layers,)),
        dma((layers,)),
        dma((layers, nz)),
        dma((layers, 2 * (nz - 1))),
        dma((layers,)),
    ]
    vmem = pl.BlockSpec(memory_space=pltpu.VMEM)
    hbm = pl.BlockSpec(memory_space=pl.ANY)
    return pl.pallas_call(
        functools.partial(kernel, dims),
        out_shape=jax.ShapeDtypeStruct(tokens.shape, BF16),
        in_specs=[vmem, vmem, vmem, vmem, hbm, hbm],
        out_specs=vmem,
        scratch_shapes=scratch,
        compiler_params=pltpu.CompilerParams(
            collective_id=0, has_side_effects=True, vmem_limit_bytes=66_000_000
        ),
    )(tokens, routes, placement, router_weight, up_weight, down_weight)


def solution(mesh, plane=8):
    return jax.shard_map(
        functools.partial(per_device, plane),
        mesh=mesh,
        in_specs=(
            P(("dp", "expert"), None),
            P(None, ("dp", "expert"), None),
            P(),
            P(None, "expert", None, "dp"),
            P(None, "expert", "dp", None),
            P(None, "expert", None),
        ),
        out_specs=P(("dp", "expert"), None),
        check_vma=False,
    )
```

```python
import functools

import jax
import jax.numpy as jnp
from jax import lax
from jax.experimental import pallas as pl
from jax.experimental.pallas import tpu as pltpu
from jax.sharding import PartitionSpec as P

MESH = pl.DeviceIdType.MESH
F32, BF16 = jnp.float32, jnp.bfloat16
NT = (((1,), (1,)), ((), ()))


def flat(value):
    width = value.shape[-1]
    return value.astype(F32).reshape(-1, width).astype(BF16)


def flat32(value):
    return value.astype(F32).reshape(-1, value.shape[-1])


def hops(direction, half, n):
    return n // 2 if (direction == 1) == (half == 0) else n // 2 - 1


def kernel(
    dims,
    tokens,
    routes,
    placement,
    router,
    up,
    down,
    out,
    stream,
    hot,
    up_w,
    down_w,
    up_v,
    down_v,
    router_v,
    zin1,
    xo1,
    rows1,
    toks2,
    xo2,
    rows2,
    h1,
    h2,
    hid1,
    hid2,
    gate1,
    gate2,
    part1,
    comb2,
    rs1o,
    rs1i,
    xr1o,
    xr1i,
    zr1o,
    zr1i,
    xr2o,
    xr2i,
    rs2o,
    rs2i,
    yr2o,
    yr2i,
    weight_sem,
    send_sem,
    z1_sem,
    x1_sem,
    ring1_sem,
    y2_sem,
    ring2_sem,
    x2_sem,
    rs1_sem,
    xr1_sem,
    zr1_sem,
    xr2_sem,
    rs2_sem,
    yr2_sem,
):
    ny, nz, nj, layers, features, w1, f2, ff = dims
    hj, hy = nj // 2, ny // 2
    y = lax.axis_index("dp")
    e = lax.axis_index("expert")
    z, j = e // nj, e % nj
    lanes = 128

    def at_y(other):
        return (other, e)

    def at_z(other):
        return (y, other * nj + j)

    def at_j(other):
        return (y, z * nj + other)

    def turn(a, n):
        return lax.rem(a + 2 * n, n)

    barrier = pltpu.get_barrier_semaphore()
    for d in range(1, ny):
        pl.semaphore_signal(barrier, inc=1, device_id=at_y(turn(y + d, ny)), device_id_type=MESH)
    for d in range(1, nz):
        pl.semaphore_signal(barrier, inc=1, device_id=at_z(turn(z + d, nz)), device_id_type=MESH)
    for d in range(1, nj):
        pl.semaphore_signal(barrier, inc=1, device_id=at_j(turn(j + d, nj)), device_id_type=MESH)

    weights = [
        pltpu.make_async_copy(up.at[0], up_w, weight_sem.at[0]),
        pltpu.make_async_copy(down.at[0], down_w, weight_sem.at[1]),
    ]
    for copy in weights:
        copy.start()

    for layer in range(layers):
        picks = routes[layer]
        count = placement.shape[1]
        names = lax.broadcasted_iota(jnp.int32, (count, picks.shape[1]), 0)
        named = jnp.zeros((count, picks.shape[1]), F32)
        for k in range(picks.shape[0]):
            named = named + jnp.where(picks[k : k + 1, :] == names, 1.0, 0.0)
        slot_of = jnp.broadcast_to(placement[layer : layer + 1, :], (lanes, count))
        slots = lax.broadcasted_iota(jnp.int32, (lanes, count), 0)
        for which, shift in ((0, 0), (1, lanes // 2)):
            serves = jnp.where(slot_of + shift == slots, 1.0, 0.0).astype(BF16)
            hot[layer, which] = lax.dot_general(
                named.astype(BF16), serves, (((0,), (1,)), ((), ())), preferred_element_type=F32
            )
    for layer in range(layers):
        gate_row = jnp.broadcast_to(router[0].astype(F32)[layer : layer + 1, :], (lanes, features)).astype(BF16)
        router_v[layer, :, 0:features] = gate_row

    stream[...] = jnp.zeros_like(stream)
    stream[:, 0:features] = tokens[...].astype(F32)

    def picker(blocks, low):
        rows = nj * blocks
        tokens_in = blocks * 8
        return rows, tokens_in, low

    def pick_matrix(hots, blocks, low):
        rows, columns, low = picker(blocks, low)
        row = lax.broadcasted_iota(jnp.int32, (rows, lanes), 0)
        slot = lax.broadcasted_iota(jnp.int32, (rows, lanes), 1)
        wanted = jnp.where(slot == low + z * nj + row // blocks, 1.0, 0.0).astype(BF16)
        same = (
            lax.broadcasted_iota(jnp.int32, (rows, columns), 0) % blocks
            == lax.broadcasted_iota(jnp.int32, (rows, columns), 1) // 8
        )
        product = lax.dot_general(wanted, hots, NT, preferred_element_type=F32)
        return jnp.where(same, product, 0.0).astype(BF16)

    def place_matrix(hots, blocks, low):
        rows, columns, low = picker(blocks, low)
        row = lax.broadcasted_iota(jnp.int32, (rows, lanes), 0)
        slot = lax.broadcasted_iota(jnp.int32, (rows, lanes), 1)
        wanted = jnp.where(slot == low + z * nj + row // blocks, 1.0, 0.0).astype(BF16)
        same = (
            lax.broadcasted_iota(jnp.int32, (columns, rows), 1) % blocks
            == lax.broadcasted_iota(jnp.int32, (columns, rows), 0) // 8
        )
        product = lax.dot_general(hots, wanted, NT, preferred_element_type=F32)
        return jnp.where(same, product, 0.0).astype(BF16)

    def send(src, dst, sent, landed, device):
        pltpu.make_async_remote_copy(
            src_ref=src, dst_ref=dst, send_sem=sent, recv_sem=landed, device_id=device, device_id_type=MESH
        ).start()

    def wait_bytes(ref, sem):
        pltpu.make_async_copy(ref, ref, sem).wait()

    (S_Z1, S_X1, S_RING1, S_Y2, S_RING2, S_X2, S_RS1, S_XR1, S_ZR1, S_XR2, S_RS2, S_YR2) = range(12)

    def layer_body(l, carry):
        sent = lambda which: send_sem.at[l, which]

        values = stream[...]
        mean = jnp.sum(values * values, axis=1, keepdims=True) * (1.0 / features)
        normed = values * lax.rsqrt(mean + 1e-05)
        zin1[l, z, :, 0:w1] = normed[:, 0:w1].astype(BF16)
        zin1[l, z, :, w1 : w1 + lanes] = hot[l, 0].astype(BF16)
        width2 = normed.shape[1] - w1
        toks2[l, z, y, :, 0 : width2 - lanes] = normed[:, w1 : w1 + width2 - lanes].astype(BF16)
        toks2[l, z, y, :, width2 - lanes : width2] = (normed[:, w1 + width2 - lanes :] + hot[l, 1]).astype(BF16)

        @pl.when(l == 0)
        def _():
            pl.semaphore_wait(barrier, ny + nz + nj - 3)

        for d in range(1, ny):
            block = toks2.at[l, z, y]
            send(block, block, sent(S_Y2), y2_sem.at[l], at_y(turn(y + d, ny)))
        for d in range(1, nz):
            block = zin1.at[l, z]
            send(block, block, sent(S_Z1), z1_sem.at[l], at_z(turn(z + d, nz)))

        @pl.when(l == 0)
        def _():
            for copy in weights:
                copy.wait()
            for layer in range(layers):
                up_v[layer] = up_w[:, layer, :]
            down_v[0] = down_w[:, 0, :]

        wait_bytes(toks2.at[l, 0, 0 : ny - 1], y2_sem.at[l])

        def ring2_send(origin, direction, half, step):
            part = toks2.at[l, origin, half * hy : (half + 1) * hy]
            send(part, part, sent(S_RING2), ring2_sem.at[l, (direction + 1) // 2, half, step - 1], at_z(turn(z + direction, nz)))

        def ring1_send(origin, direction, half, step):
            part = rows1.at[l, origin, half * hj : (half + 1) * hj]
            send(part, part, sent(S_RING1), ring1_sem.at[l, (direction + 1) // 2, half, step - 1], at_y(turn(y + direction, ny)))

        def ring_half(direction, long):
            return 0 if (direction == 1) == long else 1

        def ring2_step(step, long):
            for direction in (1, -1):
                half = ring_half(direction, long)
                origin = turn(z - direction * step, nz)
                if hops(direction, half, nz) >= step:
                    wait_bytes(
                        toks2.at[l, origin, half * hy : (half + 1) * hy],
                        ring2_sem.at[l, (direction + 1) // 2, half, step - 1],
                    )
                    if hops(direction, half, nz) > step:
                        ring2_send(origin, direction, half, step + 1)

        def ring1_step(step, long):
            for direction in (1, -1):
                half = ring_half(direction, long)
                origin = turn(y - direction * step, ny)
                if hops(direction, half, ny) >= step:
                    wait_bytes(
                        rows1.at[l, origin, half * hj : (half + 1) * hj],
                        ring1_sem.at[l, (direction + 1) // 2, half, step - 1],
                    )
                    if hops(direction, half, ny) > step:
                        ring1_send(origin, direction, half, step + 1)

        def start_ring(send_one, me, n):
            for long in (True, False):
                for direction in (1, -1):
                    half = ring_half(direction, long)
                    if hops(direction, half, n) >= 1:
                        send_one(me, direction, half, 1)

        def at_distance(me, d, n):
            return [turn(me + d, n)] if d == 0 or 2 * d == n else [turn(me + d, n), turn(me - d, n)]

        def exchange2(zc):
            chunk = flat(toks2[l, zc])
            pick = pick_matrix(chunk[:, width2 - lanes :], ny, lanes // 2)
            rows = jnp.dot(pick, chunk[:, 0:f2], preferred_element_type=F32)
            xo2[l, zc] = rows.reshape(nj, ny, f2).astype(BF16)
            rows2[l, zc, j] = xo2[l, zc, j]
            for d in range(1, nj):
                other = turn(j + d, nj)
                send(xo2.at[l, zc, other], rows2.at[l, zc, j], sent(S_X2), x2_sem.at[l, zc], at_j(other))

        def up1(yc):
            rows = flat(rows1[l, yc])
            at = pl.ds(yc * (nj * nz), nj * nz)
            result = lax.dot_general(rows, up_v[l, :, 0:w1], NT, preferred_element_type=F32)
            h1[0, at, :] = result[:, 0:lanes]
            h1[1, at, 0 : ff - lanes] = result[:, lanes:ff]
            h1[2, at, :] = lax.dot_general(rows, router_v[l, :, 0:w1], NT, preferred_element_type=F32)

        def up2(zc):
            wait_bytes(rows2.at[l, zc, 0 : nj - 1], x2_sem.at[l, zc])
            rows = flat(rows2[l, zc])
            at = pl.ds(zc * (nj * ny), nj * ny)
            result = lax.dot_general(rows, up_v[l, :, w1 : w1 + f2], NT, preferred_element_type=F32)
            h2[0, at, :] = result[:, 0:lanes]
            h2[1, at, 0 : ff - lanes] = result[:, lanes:ff]
            h2[2, at, :] = lax.dot_general(rows, router_v[l, :, w1 : w1 + f2], NT, preferred_element_type=F32)

        start_ring(ring2_send, z, nz)

        wait_bytes(zin1.at[l, 0 : nz - 1], z1_sem.at[l])
        chunk1 = flat(zin1[l])
        pick = pick_matrix(chunk1[:, w1:], nz, 0)
        picked = jnp.dot(pick, chunk1[:, 0:w1], preferred_element_type=F32)
        xo1[l] = picked.reshape(nj, nz, w1).astype(BF16)
        rows1[l, y, j] = xo1[l, j]
        for d in range(1, nj):
            other = turn(j + d, nj)
            send(xo1.at[l, other], rows1.at[l, y, j], sent(S_X1), x1_sem.at[l], at_j(other))

        exchange2(z)

        @pl.when(l == 0)
        def _():
            for layer in range(1, layers):
                down_v[layer] = down_w[:, layer, :]

        steps2, steps1 = nz // 2, ny // 2
        for step in range(1, max(steps2, steps1 + 1) + 1):
            behind = step - 1
            if step <= steps2:
                ring2_step(step, True)
            if step == 1:
                wait_bytes(rows1.at[l, y, 0 : nj - 1], x1_sem.at[l])
                start_ring(ring1_send, y, ny)
            elif behind <= steps1:
                ring1_step(behind, True)
            if step <= steps2:
                ring2_step(step, False)
                for zc in at_distance(z, step, nz):
                    exchange2(zc)
            if step == 1:
                up1(y)
            elif behind <= steps1:
                ring1_step(behind, False)
                for yc in at_distance(y, behind, ny):
                    up1(yc)
            if behind <= steps2:
                for zc in at_distance(z, behind, nz):
                    up2(zc)
        for behind in range(max(steps2, steps1 + 1), steps2 + 1):
            for zc in at_distance(z, behind, nz):
                up2(zc)

        def silu(v):
            return v / (1.0 + jnp.exp(-v))

        def sigmoid(v):
            return 1.0 / (1.0 + jnp.exp(-v))

        def join1(yc, carry):
            base = pl.multiple_of(yc * (nj * nz), nj * nz)
            total = []
            for lane in range(3):
                tiles = [
                    h2[lane, pl.ds(jc * ny + yc, nz, stride=nj * ny), :] for jc in range(nj)
                ]
                total.append(h1[lane, pl.ds(base, nj * nz), :] + jnp.concatenate(tiles, axis=0))
            hid1[yc, :, 0:lanes] = silu(total[0]).astype(BF16)
            hid1[yc, :, lanes:ff] = silu(total[1])[:, 0 : ff - lanes].astype(BF16)
            gate1[yc] = sigmoid(total[2]).astype(BF16).astype(F32)
            return carry

        def join2(zc, carry):
            base = pl.multiple_of(zc * (nj * ny), nj * ny)
            total = []
            for lane in range(3):
                tiles = [
                    h1[lane, pl.ds(jc * nz + zc, ny, stride=nj * nz), :] for jc in range(nj)
                ]
                total.append(h2[lane, pl.ds(base, nj * ny), :] + jnp.concatenate(tiles, axis=0))
            hid2[zc, :, 0:lanes] = silu(total[0]).astype(BF16)
            hid2[zc, :, lanes:ff] = silu(total[1])[:, 0 : ff - lanes].astype(BF16)
            gate2[zc] = sigmoid(total[2]).astype(BF16).astype(F32)
            return carry

        lax.fori_loop(0, nz, join2, 0)
        lax.fori_loop(0, ny, join1, 0)

        def down2(zc):
            result = jnp.dot(hid2[zc], down_v[l, :, w1 : w1 + f2], preferred_element_type=F32)
            result = result * gate2[zc][:, 0:1]
            xr2o[l, zc] = result.reshape(nj, ny, f2).astype(BF16)
            xr2i[l, zc, j] = xr2o[l, zc, j]
            for d in range(1, nj):
                other = turn(j + d, nj)
                send(xr2o.at[l, zc, other], xr2i.at[l, zc, j], sent(S_XR2), xr2_sem.at[l, zc], at_j(other))

        def down1(yc):
            result = jnp.dot(hid1[yc], down_v[l, :, 0:w1], preferred_element_type=F32)
            result = result * gate1[yc][:, 0:1]
            part1[yc] = result.reshape(nj, nz, w1).astype(BF16)

        def combine2(zc):
            wait_bytes(xr2i.at[l, zc, 0 : nj - 1], xr2_sem.at[l, zc])
            place = place_matrix(flat(toks2[l, zc, :, :, width2 - lanes :]), ny, lanes // 2)
            total = jnp.dot(place, flat(xr2i[l, zc]), preferred_element_type=F32)
            comb2[zc] = total.reshape(ny, 8, f2).astype(BF16)

        def slot_of_send(moving, half, step, n):
            long, short = n // 2, n // 2 - 1
            order = []
            for m in (1, -1):
                for h in (0, 1):
                    for s in range(1, hops(-m, h, n) + 1):
                        order.append((m, h, s))
            return order.index((moving, half, step))

        def reduce_step(me, n, size, own, outgoing, incoming, sems, sent_sem, to, step, long):
            for moving in (1, -1):
                half = ring_half(-moving, long)
                length = hops(-moving, half, n)
                if length < step:
                    continue
                dest = turn(me + moving * (length + 1 - step), n)
                value = own[dest, half * size : (half + 1) * size]
                slot = slot_of_send(moving, half, step, n)
                if step > 1:
                    before = slot_of_send(moving, half, step - 1, n)
                    wait_bytes(incoming.at[l, before], sems.at[l, before])
                    value = (value.astype(F32) + incoming[l, before].astype(F32)).astype(BF16)
                outgoing[l, slot] = value
                send(outgoing.at[l, slot], incoming.at[l, slot], sent_sem, sems.at[l, slot], to(turn(me + moving, n)))

        def reduce_end(me, n, size, own, incoming, sems):
            halves = []
            for half in (0, 1):
                total = own[me, half * size : (half + 1) * size].astype(F32)
                for moving in (1, -1):
                    length = hops(-moving, half, n)
                    if length >= 1:
                        slot = slot_of_send(moving, half, length, n)
                        wait_bytes(incoming.at[l, slot], sems.at[l, slot])
                        total = total + incoming[l, slot].astype(F32)
                halves.append(total)
            return halves

        def reduce1(step, long):
            reduce_step(y, ny, hj, part1, rs1o, rs1i, rs1_sem, sent(S_RS1), at_y, step, long)

        def reduce2(step, long):
            reduce_step(z, nz, hy, comb2, rs2o, rs2i, rs2_sem, sent(S_RS2), at_z, step, long)

        def finish1():
            for half, total in enumerate(reduce_end(y, ny, hj, part1, rs1i, rs1_sem)):
                xr1o[l, half * hj : (half + 1) * hj, :, 0:w1] = total.astype(BF16)
            xr1o[l, :, :, w1 : w1 + lanes] = gate1[y].reshape(nj, nz, lanes).astype(BF16)
            xr1i[l, j] = xr1o[l, j]
            for d in range(1, nj):
                other = turn(j + d, nj)
                send(xr1o.at[l, other], xr1i.at[l, j], sent(S_XR1), xr1_sem.at[l], at_j(other))

        combined = set()

        def need2(distance):
            for zc_at, zc in enumerate(at_distance(z, distance, nz)):
                if (distance, zc_at) not in combined:
                    combined.add((distance, zc_at))
                    combine2(zc)

        for d in range(steps2, steps2 - 2, -1):
            for zc in at_distance(z, d, nz):
                down2(zc)
            if steps1 - steps2 + d >= 0:
                for yc in at_distance(y, steps1 - steps2 + d, ny):
                    down1(yc)
            reduce1(1, d == steps2)
        for d in range(steps2 - 2, -1, -1):
            for zc in at_distance(z, d, nz):
                down2(zc)
        for d in range(steps1 - 2, -1, -1):
            for yc in at_distance(y, d, ny):
                down1(yc)
        for step in range(1, max(steps1, steps2) + 1):
            reduce1(step + 1, True)
            if step <= steps2:
                need2(steps2 + 1 - step)
                reduce2(step, True)
            if step == steps1 - 1:
                finish1()
            reduce1(step + 1, False)
            if step < steps2:
                need2(steps2 - step)
                reduce2(step, False)
        if steps1 == 1:
            finish1()
        need2(0)

        wait_bytes(xr1i.at[l, 0 : nj - 1], xr1_sem.at[l])
        place1 = place_matrix(flat(zin1[l, :, :, w1 : w1 + lanes]), nz, 0)
        sums = jnp.dot(place1, flat(xr1i[l]), preferred_element_type=F32)
        zr1o[l, :, :, 0:w1] = sums[:, 0:w1].reshape(nz, 8, w1).astype(BF16)
        gates = sums[:, w1:]
        high = gates.astype(BF16).astype(F32)
        lane = lax.broadcasted_iota(jnp.int32, gates.shape, 1)
        pair = jnp.where(lane < lanes // 2, high, gates - high)
        zr1o[l, :, :, w1 : w1 + lanes] = pair.reshape(nz, 8, lanes).astype(BF16)
        zr1i[l, z] = zr1o[l, z]
        for d in range(1, nz):
            other = turn(z + d, nz)
            send(zr1o.at[l, other], zr1i.at[l, z], sent(S_ZR1), zr1_sem.at[l], at_z(other))

        for half, total in enumerate(reduce_end(z, nz, hy, comb2, rs2i, rs2_sem)):
            yr2o[l, half * hy : (half + 1) * hy] = total.astype(BF16)
        yr2i[l, y] = yr2o[l, y]
        for d in range(1, ny):
            other = turn(y + d, ny)
            send(yr2o.at[l, other], yr2i.at[l, y], sent(S_YR2), yr2_sem.at[l], at_y(other))

        wait_bytes(yr2i.at[l, 0 : ny - 1], yr2_sem.at[l])
        numer2 = jnp.sum(yr2i[l].astype(F32), axis=0)
        wait_bytes(zr1i.at[l, 0 : nz - 1], zr1_sem.at[l])
        both = jnp.sum(zr1i[l].astype(F32), axis=0)
        denom = both[:, w1 : w1 + 1] + both[:, w1 + lanes // 2 : w1 + lanes // 2 + 1]
        denom = jnp.maximum(denom, 0.5)
        stream[:, 0:w1] = (stream[:, 0:w1] + both[:, 0:w1] / denom).astype(BF16).astype(F32)
        stream[:, w1 : w1 + f2] = (stream[:, w1 : w1 + f2] + numer2 / denom).astype(BF16).astype(F32)

        wait_bytes(zin1.at[l, 0 : nz - 1], sent(S_Z1))
        wait_bytes(xo1.at[l, 0 : nj - 1], sent(S_X1))
        wait_bytes(rows1.at[l, 0 : ny - 1], sent(S_RING1))
        wait_bytes(toks2.at[l, 0, 0 : ny - 1], sent(S_Y2))
        wait_bytes(toks2.at[l, 0 : nz - 1], sent(S_RING2))
        wait_bytes(xo2.at[l, :, 0 : nj - 1], sent(S_X2))
        wait_bytes(rs1o.at[l], sent(S_RS1))
        wait_bytes(xr1o.at[l, 0 : nj - 1], sent(S_XR1))
        wait_bytes(zr1o.at[l, 0 : nz - 1], sent(S_ZR1))
        wait_bytes(xr2o.at[l, :, 0 : nj - 1], sent(S_XR2))
        wait_bytes(rs2o.at[l], sent(S_RS2))
        wait_bytes(yr2o.at[l, 0 : ny - 1], sent(S_YR2))
        return carry

    lax.fori_loop(0, layers, layer_body, 0)
    out[...] = stream[:, 0:features].astype(BF16)


def per_device(plane, tokens, routes, placement, up_weight, down_weight, router_weight):
    ny = lax.axis_size("dp")
    nj = plane
    nz = lax.axis_size("expert") // nj
    layers, _, features, ff = up_weight.shape
    w1 = features // 256 * 128 + (128 if features > 1024 else 0)
    f2 = features - w1
    padded = -(-features // 128) * 128
    width2 = padded - w1
    hj, hy = nj // 2, ny // 2
    dims = (ny, nz, nj, layers, features, w1, f2, ff)
    rows = ny * nz * nj
    dma = pltpu.SemaphoreType.DMA
    scratch = [
        pltpu.VMEM((8, padded), F32),
        pltpu.VMEM((layers, 2, 8, 128), F32),
        pltpu.VMEM((ff, layers, features), BF16),
        pltpu.VMEM((ff, layers, features), BF16),
        pltpu.VMEM((layers, ff, features), BF16),
        pltpu.VMEM((layers, ff, features), BF16),
        pltpu.VMEM((layers, 128, features), BF16),
        pltpu.VMEM((layers, nz, 8, w1 + 128), BF16),
        pltpu.VMEM((layers, nj, nz, w1), BF16),
        pltpu.VMEM((layers, ny, nj, nz, w1), BF16),
        pltpu.VMEM((layers, nz, ny, 8, width2), BF16),
        pltpu.VMEM((layers, nz, nj, ny, f2), BF16),
        pltpu.VMEM((layers, nz, nj, ny, f2), BF16),
        pltpu.VMEM((3, rows, 128), F32),
        pltpu.VMEM((3, rows, 128), F32),
        pltpu.VMEM((ny, nj * nz, ff), BF16),
        pltpu.VMEM((nz, nj * ny, ff), BF16),
        pltpu.VMEM((ny, nj * nz, 128), F32),
        pltpu.VMEM((nz, nj * ny, 128), F32),
        pltpu.VMEM((ny, nj, nz, w1), BF16),
        pltpu.VMEM((nz, ny, 8, f2), BF16),
        pltpu.VMEM((layers, 2 * (ny - 1), hj, nz, w1), BF16),
        pltpu.VMEM((layers, 2 * (ny - 1), hj, nz, w1), BF16),
        pltpu.VMEM((layers, nj, nz, w1 + 128), BF16),
        pltpu.VMEM((layers, nj, nz, w1 + 128), BF16),
        pltpu.VMEM((layers, nz, 8, w1 + 128), BF16),
        pltpu.VMEM((layers, nz, 8, w1 + 128), BF16),
        pltpu.VMEM((layers, nz, nj, ny, f2), BF16),
        pltpu.VMEM((layers, nz, nj, ny, f2), BF16),
        pltpu.VMEM((layers, 2 * (nz - 1), hy, 8, f2), BF16),
        pltpu.VMEM((layers, 2 * (nz - 1), hy, 8, f2), BF16),
        pltpu.VMEM((layers, ny, 8, f2), BF16),
        pltpu.VMEM((layers, ny, 8, f2), BF16),
        dma((2,)),
        dma((layers, 12)),
        dma((layers,)),
        dma((layers,)),
        dma((layers, 2, 2, ny // 2)),
        dma((layers,)),
        dma((layers, 2, 2, nz // 2)),
        dma((layers, nz)),
        dma((layers, 2 * (ny - 1))),
        dma((layers,)),
        dma((layers,)),
        dma((layers, nz)),
        dma((layers, 2 * (nz - 1))),
        dma((layers,)),
    ]
    vmem = pl.BlockSpec(memory_space=pltpu.VMEM)
    hbm = pl.BlockSpec(memory_space=pl.ANY)
    return pl.pallas_call(
        functools.partial(kernel, dims),
        out_shape=jax.ShapeDtypeStruct(tokens.shape, BF16),
        in_specs=[vmem, vmem, vmem, vmem, hbm, hbm],
        out_specs=vmem,
        scratch_shapes=scratch,
        compiler_params=pltpu.CompilerParams(
            collective_id=0, has_side_effects=True, vmem_limit_bytes=66_000_000
        ),
    )(
        tokens,
        jnp.transpose(routes, (0, 2, 1)),
        placement,
        jnp.transpose(router_weight, (1, 0, 2)),
        jnp.transpose(up_weight, (1, 3, 0, 2)),
        jnp.transpose(down_weight, (1, 2, 0, 3)),
    )


def solution(mesh, plane=8):
    return jax.shard_map(
        functools.partial(per_device, plane),
        mesh=mesh,
        in_specs=(
            P(("dp", "expert"), None),
            P(None, ("dp", "expert"), None),
            P(),
            P(None, "expert", None, "dp"),
            P(None, "expert", "dp", None),
            P(None, "expert", None),
        ),
        out_specs=P(("dp", "expert"), None),
        check_vma=False,
    )
```

```python
import functools

import jax
import jax.numpy as jnp
from jax import lax
from jax.experimental import pallas as pl
from jax.experimental.pallas import tpu as pltpu
from jax.sharding import PartitionSpec as P

MESH = pl.DeviceIdType.MESH
F32, BF16 = jnp.float32, jnp.bfloat16
NT = (((1,), (1,)), ((), ()))


def flat(value):
    width = value.shape[-1]
    return value.astype(F32).reshape(-1, width).astype(BF16)


def flat32(value):
    return value.astype(F32).reshape(-1, value.shape[-1])


def hops(direction, half, n):
    return n // 2 if (direction == 1) == (half == 0) else n // 2 - 1


def kernel(
    dims,
    tokens,
    routes,
    placement,
    router,
    up,
    down,
    out,
    stream,
    hot,
    up_w,
    down_w,
    up_v,
    down_v,
    router_v,
    h1,
    h2,
    hid1,
    hid2,
    gate1,
    gate2,
    zin1,
    xo1,
    rows1,
    part1,
    rs1o,
    rs1i,
    xr1o,
    xr1i,
    zr1o,
    zr1i,
    toks2,
    xo2,
    rows2,
    comb2,
    xr2o,
    xr2i,
    rs2o,
    rs2i,
    yr2o,
    yr2i,
    weight_sem,
    send_sem,
    z1_sem,
    x1_sem,
    ring1_sem,
    y2_sem,
    ring2_sem,
    x2_sem,
    rs1_sem,
    xr1_sem,
    zr1_sem,
    xr2_sem,
    rs2_sem,
    yr2_sem,
):
    ny, nz, nj, layers, features, cuts1, cuts2, ff = dims
    hj, hy = nj // 2, ny // 2
    y = lax.axis_index("dp")
    e = lax.axis_index("expert")
    z, j = e // nj, e % nj
    lanes = 128

    def at_y(other):
        return (other, e)

    def at_z(other):
        return (y, other * nj + j)

    def at_j(other):
        return (y, z * nj + other)

    def turn(a, n):
        return lax.rem(a + 2 * n, n)

    barrier = pltpu.get_barrier_semaphore()
    for d in range(1, ny):
        pl.semaphore_signal(barrier, inc=1, device_id=at_y(turn(y + d, ny)), device_id_type=MESH)
    for d in range(1, nz):
        pl.semaphore_signal(barrier, inc=1, device_id=at_z(turn(z + d, nz)), device_id_type=MESH)
    for d in range(1, nj):
        pl.semaphore_signal(barrier, inc=1, device_id=at_j(turn(j + d, nj)), device_id_type=MESH)

    weights = [
        pltpu.make_async_copy(up.at[0], up_w, weight_sem.at[0]),
        pltpu.make_async_copy(down.at[0], down_w, weight_sem.at[1]),
    ]
    for copy in weights:
        copy.start()

    for layer in range(layers):
        picks = routes[layer]
        count = placement.shape[1]
        names = lax.broadcasted_iota(jnp.int32, (count, picks.shape[1]), 0)
        named = jnp.zeros((count, picks.shape[1]), F32)
        for k in range(picks.shape[0]):
            named = named + jnp.where(picks[k : k + 1, :] == names, 1.0, 0.0)
        slot_of = jnp.broadcast_to(placement[layer : layer + 1, :], (lanes, count))
        slots = lax.broadcasted_iota(jnp.int32, (lanes, count), 0)
        for which, shift in ((0, 0), (1, lanes // 2)):
            serves = jnp.where(slot_of + shift == slots, 1.0, 0.0).astype(BF16)
            hot[layer, which] = lax.dot_general(
                named.astype(BF16), serves, (((0,), (1,)), ((), ())), preferred_element_type=F32
            )
    for layer in range(layers):
        gate_row = jnp.broadcast_to(router[0].astype(F32)[layer : layer + 1, :], (lanes, features)).astype(BF16)
        router_v[layer, :, 0:features] = gate_row

    stream[...] = jnp.zeros_like(stream)
    stream[:, 0:features] = tokens[...].astype(F32)

    def picker(blocks, low):
        rows = nj * blocks
        tokens_in = blocks * 8
        return rows, tokens_in, low

    def pick_matrix(hots, blocks, low):
        rows, columns, low = picker(blocks, low)
        row = lax.broadcasted_iota(jnp.int32, (rows, lanes), 0)
        slot = lax.broadcasted_iota(jnp.int32, (rows, lanes), 1)
        wanted = jnp.where(slot == low + z * nj + row // blocks, 1.0, 0.0).astype(BF16)
        same = (
            lax.broadcasted_iota(jnp.int32, (rows, columns), 0) % blocks
            == lax.broadcasted_iota(jnp.int32, (rows, columns), 1) // 8
        )
        product = lax.dot_general(wanted, hots, NT, preferred_element_type=F32)
        return jnp.where(same, product, 0.0).astype(BF16)

    def place_matrix(hots, blocks, low):
        rows, columns, low = picker(blocks, low)
        row = lax.broadcasted_iota(jnp.int32, (rows, lanes), 0)
        slot = lax.broadcasted_iota(jnp.int32, (rows, lanes), 1)
        wanted = jnp.where(slot == low + z * nj + row // blocks, 1.0, 0.0).astype(BF16)
        same = (
            lax.broadcasted_iota(jnp.int32, (columns, rows), 1) % blocks
            == lax.broadcasted_iota(jnp.int32, (columns, rows), 0) // 8
        )
        product = lax.dot_general(hots, wanted, NT, preferred_element_type=F32)
        return jnp.where(same, product, 0.0).astype(BF16)

    def send(src, dst, sent, landed, device):
        pltpu.make_async_remote_copy(
            src_ref=src, dst_ref=dst, send_sem=sent, recv_sem=landed, device_id=device, device_id_type=MESH
        ).start()

    def wait_bytes(ref, sem):
        pltpu.make_async_copy(ref, ref, sem).wait()

    (S_Z1, S_X1, S_RING1, S_Y2, S_RING2, S_X2, S_RS1, S_XR1, S_ZR1, S_XR2, S_RS2, S_YR2) = range(12)

    parts = (0, 1)

    def layer_body(l, carry):
        sent = lambda which, part: send_sem.at[l, which, part]

        values = stream[...]
        mean = jnp.sum(values * values, axis=1, keepdims=True) * (1.0 / features)
        normed = values * lax.rsqrt(mean + 1e-05)
        for p in parts:
            low, high = cuts1[p]
            zin1[p][l, z, :, 0 : high - low] = normed[:, low:high].astype(BF16)
            if p == 0:
                zin1[p][l, z, :, high - low : high - low + lanes] = hot[l, 0].astype(BF16)
            low, high = cuts2[p]
            if p == 0:
                full = (high - low) // lanes * lanes
                toks2[p][l, z, y, :, 0:full] = normed[:, low : low + full].astype(BF16)
                toks2[p][l, z, y, :, full : full + lanes] = (normed[:, low + full :] + hot[l, 1]).astype(BF16)
            else:
                toks2[p][l, z, y] = normed[:, low:high].astype(BF16)

        @pl.when(l == 0)
        def _():
            pl.semaphore_wait(barrier, ny + nz + nj - 3)

        for p in parts:
            for d in range(1, ny):
                block = toks2[p].at[l, z, y]
                send(block, block, sent(S_Y2, p), y2_sem.at[l, p], at_y(turn(y + d, ny)))
            for d in range(1, nz):
                block = zin1[p].at[l, z]
                send(block, block, sent(S_Z1, p), z1_sem.at[l, p], at_z(turn(z + d, nz)))

        @pl.when(l == 0)
        def _():
            for copy in weights:
                copy.wait()
            up_v[0] = up_w[:, 0, :]
            down_v[0] = down_w[:, 0, :]

        def ring_half(direction, long):
            return 0 if (direction == 1) == long else 1

        def ring2_send(origin, direction, half, step, p):
            part = toks2[p].at[l, origin, half * hy : (half + 1) * hy]
            landed = ring2_sem.at[l, p, (direction + 1) // 2, half, step - 1]
            send(part, part, sent(S_RING2, p), landed, at_z(turn(z + direction, nz)))

        def ring1_send(origin, direction, half, step, p):
            part = rows1[p].at[l, origin, half * hj : (half + 1) * hj]
            landed = ring1_sem.at[l, p, (direction + 1) // 2, half, step - 1]
            send(part, part, sent(S_RING1, p), landed, at_y(turn(y + direction, ny)))

        def ring2_step(step, p, long):
            for direction in (1, -1):
                half = ring_half(direction, long)
                origin = turn(z - direction * step, nz)
                if hops(direction, half, nz) >= step:
                    part = toks2[p].at[l, origin, half * hy : (half + 1) * hy]
                    wait_bytes(part, ring2_sem.at[l, p, (direction + 1) // 2, half, step - 1])
                    if hops(direction, half, nz) > step:
                        ring2_send(origin, direction, half, step + 1, p)

        def ring1_step(step, p, long):
            for direction in (1, -1):
                half = ring_half(direction, long)
                origin = turn(y - direction * step, ny)
                if hops(direction, half, ny) >= step:
                    part = rows1[p].at[l, origin, half * hj : (half + 1) * hj]
                    wait_bytes(part, ring1_sem.at[l, p, (direction + 1) // 2, half, step - 1])
                    if hops(direction, half, ny) > step:
                        ring1_send(origin, direction, half, step + 1, p)

        def start_ring(send_one, me, n, p):
            for long in (True, False):
                for direction in (1, -1):
                    half = ring_half(direction, long)
                    if hops(direction, half, n) >= 1:
                        send_one(me, direction, half, 1, p)

        def at_distance(me, d, n):
            return [turn(me + d, n)] if d == 0 or 2 * d == n else [turn(me + d, n), turn(me - d, n)]

        kept = {}

        def hots2(zc):
            width = cuts2[0][1] - cuts2[0][0]
            full = width // lanes * lanes
            return flat(toks2[0][l, zc, :, :, full : full + lanes])

        def exchange2(distance, p):
            for at, zc in enumerate(at_distance(z, distance, nz)):
                if p == 0:
                    kept["pick", distance, at] = pick_matrix(hots2(zc), ny, lanes // 2)
                width = cuts2[p][1] - cuts2[p][0]
                tokens_in = flat(toks2[p][l, zc, :, :, 0:width])
                rows = jnp.dot(kept["pick", distance, at], tokens_in, preferred_element_type=F32)
                xo2[p][l, zc] = rows.reshape(nj, ny, width).astype(BF16)
                rows2[p][l, zc, j] = xo2[p][l, zc, j]
                for d in range(1, nj):
                    other = turn(j + d, nj)
                    send(xo2[p].at[l, zc, other], rows2[p].at[l, zc, j], sent(S_X2, p), x2_sem.at[l, p, zc], at_j(other))

        def products(rows, cuts):
            hidden, gate = 0.0, 0.0
            for p in parts:
                low, high = cuts[p]
                hidden += lax.dot_general(rows[p], up_v[l, :, low:high], NT, preferred_element_type=F32)
                gate += lax.dot_general(rows[p], router_v[l, :, low:high], NT, preferred_element_type=F32)
            return hidden[:, 0:lanes], hidden[:, lanes:ff], gate

        def up1(yc):
            at = pl.ds(yc * (nj * nz), nj * nz)
            first, second, gate = products([flat(rows1[p][l, yc]) for p in parts], cuts1)
            h1[0, at, :] = first
            h1[1, at, 0 : ff - lanes] = second
            h1[2, at, :] = gate

        def up2(zc):
            for p in parts:
                wait_bytes(rows2[p].at[l, zc, 0 : nj - 1], x2_sem.at[l, p, zc])
            at = pl.ds(zc * (nj * ny), nj * ny)
            first, second, gate = products([flat(rows2[p][l, zc]) for p in parts], cuts2)
            h2[0, at, :] = first
            h2[1, at, 0 : ff - lanes] = second
            h2[2, at, :] = gate

        hots1 = None
        for p in parts:
            wait_bytes(toks2[p].at[l, 0, 0 : ny - 1], y2_sem.at[l, p])
            start_ring(ring2_send, z, nz, p)
            wait_bytes(zin1[p].at[l, 0 : nz - 1], z1_sem.at[l, p])
            width = cuts1[p][1] - cuts1[p][0]
            if p == 0:
                hots1 = flat(zin1[p][l, :, :, width : width + lanes])
                pick1 = pick_matrix(hots1, nz, 0)
            picked = jnp.dot(pick1, flat(zin1[p][l, :, :, 0:width]), preferred_element_type=F32)
            xo1[p][l] = picked.reshape(nj, nz, width).astype(BF16)
            rows1[p][l, y, j] = xo1[p][l, j]
            for d in range(1, nj):
                other = turn(j + d, nj)
                send(xo1[p].at[l, other], rows1[p].at[l, y, j], sent(S_X1, p), x1_sem.at[l, p], at_j(other))
        for p in parts:
            exchange2(0, p)

        steps2, steps1 = nz // 2, ny // 2
        for step in range(1, max(steps2, steps1 + 1) + 1):
            behind = step - 1
            for p in parts:
                if step <= steps2:
                    ring2_step(step, p, True)
                if step == 1:
                    wait_bytes(rows1[p].at[l, y, 0 : nj - 1], x1_sem.at[l, p])
                    start_ring(ring1_send, y, ny, p)
                elif behind <= steps1:
                    ring1_step(behind, p, True)
                if step <= steps2:
                    ring2_step(step, p, False)
                    exchange2(step, p)
                if 1 <= behind <= steps1:
                    ring1_step(behind, p, False)
            if behind <= steps1:
                for yc in at_distance(y, behind, ny):
                    up1(yc)
            if behind <= steps2:
                for zc in at_distance(z, behind, nz):
                    up2(zc)
        for behind in range(max(steps2, steps1 + 1), steps2 + 1):
            for zc in at_distance(z, behind, nz):
                up2(zc)

        def silu(v):
            return v / (1.0 + jnp.exp(-v))

        def sigmoid(v):
            return 1.0 / (1.0 + jnp.exp(-v))

        def join(chunk, own, other, ours, theirs, hidden, gate):
            base = pl.multiple_of(chunk * (nj * theirs), nj * theirs)
            total = []
            for lane in range(3):
                tiles = [other[lane, pl.ds(jc * ours + chunk, theirs, stride=nj * ours), :] for jc in range(nj)]
                total.append(own[lane, pl.ds(base, nj * theirs), :] + jnp.concatenate(tiles, axis=0))
            hidden[chunk, :, 0:lanes] = silu(total[0]).astype(BF16)
            hidden[chunk, :, lanes:ff] = silu(total[1])[:, 0 : ff - lanes].astype(BF16)
            gate[chunk] = sigmoid(total[2]).astype(BF16).astype(F32)

        def down2(distance):
            for zc in at_distance(z, distance, nz):
                join(zc, h2, h1, nz, ny, hid2, gate2)
                for p in parts:
                    low, high = cuts2[p]
                    result = jnp.dot(hid2[zc], down_v[l, :, low:high], preferred_element_type=F32)
                    result = result * gate2[zc][:, 0:1]
                    xr2o[p][l, zc] = result.reshape(nj, ny, high - low).astype(BF16)
                    xr2i[p][l, zc, j] = xr2o[p][l, zc, j]
                    for d in range(1, nj):
                        other = turn(j + d, nj)
                        send(
                            xr2o[p].at[l, zc, other], xr2i[p].at[l, zc, j], sent(S_XR2, p), xr2_sem.at[l, p, zc], at_j(other)
                        )

        def down1(distance):
            if ("part", distance) in kept or distance < 0:
                return
            kept["part", distance] = True
            for yc in at_distance(y, distance, ny):
                join(yc, h1, h2, ny, nz, hid1, gate1)
                for p in parts:
                    low, high = cuts1[p]
                    result = jnp.dot(hid1[yc], down_v[l, :, low:high], preferred_element_type=F32)
                    result = result * gate1[yc][:, 0:1]
                    part1[p][yc] = result.reshape(nj, nz, high - low).astype(BF16)

        def need2(distance, p):
            for at, zc in enumerate(at_distance(z, distance, nz)):
                if ("sum", distance, at, p) in kept:
                    continue
                kept["sum", distance, at, p] = True
                if p == 0:
                    kept["place", distance, at] = place_matrix(hots2(zc), ny, lanes // 2)
                wait_bytes(xr2i[p].at[l, zc, 0 : nj - 1], xr2_sem.at[l, p, zc])
                total = jnp.dot(kept["place", distance, at], flat(xr2i[p][l, zc]), preferred_element_type=F32)
                comb2[p][zc] = total.reshape(ny, 8, total.shape[1]).astype(BF16)

        def slot_of_send(moving, half, step, n):
            order = []
            for m in (1, -1):
                for h in (0, 1):
                    for s in range(1, hops(-m, h, n) + 1):
                        order.append((m, h, s))
            return order.index((moving, half, step))

        def reduce_step(me, n, size, own, outgoing, incoming, sems, sent_sem, to, step, long):
            for moving in (1, -1):
                half = ring_half(-moving, long)
                length = hops(-moving, half, n)
                if length < step:
                    continue
                dest = turn(me + moving * (length + 1 - step), n)
                value = own[dest, half * size : (half + 1) * size]
                slot = slot_of_send(moving, half, step, n)
                if step > 1:
                    before = slot_of_send(moving, half, step - 1, n)
                    wait_bytes(incoming.at[l, before], sems(before))
                    value = (value.astype(F32) + incoming[l, before].astype(F32)).astype(BF16)
                outgoing[l, slot] = value
                send(outgoing.at[l, slot], incoming.at[l, slot], sent_sem, sems(slot), to(turn(me + moving, n)))

        def reduce_end(me, n, size, own, incoming, sems):
            halves = []
            for half in (0, 1):
                total = own[me, half * size : (half + 1) * size].astype(F32)
                for moving in (1, -1):
                    length = hops(-moving, half, n)
                    if length >= 1:
                        slot = slot_of_send(moving, half, length, n)
                        wait_bytes(incoming.at[l, slot], sems(slot))
                        total = total + incoming[l, slot].astype(F32)
                halves.append(total)
            return halves

        def reduce1(step, p, long):
            reduce_step(
                y, ny, hj, part1[p], rs1o[p], rs1i[p], lambda slot: rs1_sem.at[l, p, slot], sent(S_RS1, p), at_y, step, long
            )

        def reduce2(step, p, long):
            reduce_step(
                z, nz, hy, comb2[p], rs2o[p], rs2i[p], lambda slot: rs2_sem.at[l, p, slot], sent(S_RS2, p), at_z, step, long
            )

        def finish1(p):
            width = cuts1[p][1] - cuts1[p][0]
            ended = reduce_end(y, ny, hj, part1[p], rs1i[p], lambda slot: rs1_sem.at[l, p, slot])
            for half, total in enumerate(ended):
                xr1o[p][l, half * hj : (half + 1) * hj, :, 0:width] = total.astype(BF16)
            if p == 0:
                xr1o[p][l, :, :, width : width + lanes] = gate1[y].reshape(nj, nz, lanes).astype(BF16)
            xr1i[p][l, j] = xr1o[p][l, j]
            for d in range(1, nj):
                other = turn(j + d, nj)
                send(xr1o[p].at[l, other], xr1i[p].at[l, j], sent(S_XR1, p), xr1_sem.at[l, p], at_j(other))

        for d in range(steps2, steps2 - 2, -1):
            down2(d)
            down1(steps1 - steps2 + d)
            for p in parts:
                reduce1(1, p, d == steps2)
        for d in range(steps2 - 2, -1, -1):
            down2(d)
        for step in range(1, max(steps1, steps2) + 1):
            for long in (True, False):
                if step == max(steps1 - 1, 1):
                    down1(0)
                down1(steps1 - step if long else steps1 - 1 - step)
                for p in parts:
                    reduce1(step + 1, p, long)
                    distance = steps2 + 1 - step if long else steps2 - step
                    if distance >= 1:
                        need2(distance, p)
                        reduce2(step, p, long)
                if step == max(steps1 - 1, 1):
                    finish1(0 if long else 1)
        for p in parts:
            need2(0, p)

        place1 = place_matrix(flat(zin1[0][l, :, :, cuts1[0][1] : cuts1[0][1] + lanes]), nz, 0)
        for p in parts:
            width = cuts1[p][1] - cuts1[p][0]
            wait_bytes(xr1i[p].at[l, 0 : nj - 1], xr1_sem.at[l, p])
            sums = jnp.dot(place1, flat(xr1i[p][l]), preferred_element_type=F32)
            zr1o[p][l, :, :, 0:width] = sums[:, 0:width].reshape(nz, 8, width).astype(BF16)
            if p == 0:
                gates = sums[:, width:]
                rounded = gates.astype(BF16).astype(F32)
                lane = lax.broadcasted_iota(jnp.int32, gates.shape, 1)
                pair = jnp.where(lane < lanes // 2, rounded, gates - rounded)
                zr1o[p][l, :, :, width : width + lanes] = pair.reshape(nz, 8, lanes).astype(BF16)
            zr1i[p][l, z] = zr1o[p][l, z]
            for d in range(1, nz):
                other = turn(z + d, nz)
                send(zr1o[p].at[l, other], zr1i[p].at[l, z], sent(S_ZR1, p), zr1_sem.at[l, p], at_z(other))

            ended = reduce_end(z, nz, hy, comb2[p], rs2i[p], lambda slot: rs2_sem.at[l, p, slot])
            for half, total in enumerate(ended):
                yr2o[p][l, half * hy : (half + 1) * hy] = total.astype(BF16)
            yr2i[p][l, y] = yr2o[p][l, y]
            for d in range(1, ny):
                other = turn(y + d, ny)
                send(yr2o[p].at[l, other], yr2i[p].at[l, y], sent(S_YR2, p), yr2_sem.at[l, p], at_y(other))

        @pl.when(l == 0)
        def _():
            for layer in range(1, layers):
                up_v[layer] = up_w[:, layer, :]
                down_v[layer] = down_w[:, layer, :]

        denom = None
        for p in parts:
            low, high = cuts1[p]
            wait_bytes(zr1i[p].at[l, 0 : nz - 1], zr1_sem.at[l, p])
            both = jnp.sum(zr1i[p][l].astype(F32), axis=0)
            if p == 0:
                width = high - low
                denom = both[:, width : width + 1] + both[:, width + lanes // 2 : width + lanes // 2 + 1]
                denom = jnp.maximum(denom, 0.5)
            stream[:, low:high] = (stream[:, low:high] + both[:, 0 : high - low] / denom).astype(BF16).astype(F32)
            low, high = cuts2[p]
            wait_bytes(yr2i[p].at[l, 0 : ny - 1], yr2_sem.at[l, p])
            numer = jnp.sum(yr2i[p][l].astype(F32), axis=0)
            stream[:, low:high] = (stream[:, low:high] + numer / denom).astype(BF16).astype(F32)

        for p in parts:
            wait_bytes(zin1[p].at[l, 0 : nz - 1], sent(S_Z1, p))
            wait_bytes(xo1[p].at[l, 0 : nj - 1], sent(S_X1, p))
            wait_bytes(rows1[p].at[l, 0 : ny - 1], sent(S_RING1, p))
            wait_bytes(toks2[p].at[l, 0, 0 : ny - 1], sent(S_Y2, p))
            wait_bytes(toks2[p].at[l, 0 : nz - 1], sent(S_RING2, p))
            wait_bytes(xo2[p].at[l, :, 0 : nj - 1], sent(S_X2, p))
            wait_bytes(rs1o[p].at[l], sent(S_RS1, p))
            wait_bytes(xr1o[p].at[l, 0 : nj - 1], sent(S_XR1, p))
            wait_bytes(zr1o[p].at[l, 0 : nz - 1], sent(S_ZR1, p))
            wait_bytes(xr2o[p].at[l, :, 0 : nj - 1], sent(S_XR2, p))
            wait_bytes(rs2o[p].at[l], sent(S_RS2, p))
            wait_bytes(yr2o[p].at[l, 0 : ny - 1], sent(S_YR2, p))
        return carry

    lax.fori_loop(0, layers, layer_body, 0)
    out[...] = stream[:, 0:features].astype(BF16)


def per_device(plane, tokens, routes, placement, up_weight, down_weight, router_weight):
    ny = lax.axis_size("dp")
    nj = plane
    nz = lax.axis_size("expert") // nj
    layers, _, features, ff = up_weight.shape
    tiles = features // 128
    tiles1 = tiles // 2 + (1 if tiles > 8 else 0)
    first1 = tiles1 // 2 * 128
    w1 = tiles1 * 128
    second2 = w1 + (tiles - tiles1) // 2 * 128
    cuts1 = ((0, first1), (first1, w1))
    cuts2 = ((second2, features), (w1, second2))
    padded = -(-features // 128) * 128
    hj, hy = nj // 2, ny // 2
    dims = (ny, nz, nj, layers, features, cuts1, cuts2, ff)
    rows = ny * nz * nj
    dma = pltpu.SemaphoreType.DMA
    data1 = [high - low for low, high in cuts1]
    wide1 = [data1[0] + 128, data1[1]]
    data2 = [high - low for low, high in cuts2]
    wide2 = [padded - second2, data2[1]]

    def buffers(shape, widths):
        return [pltpu.VMEM((*shape, width), BF16) for width in widths]

    scratch = [
        pltpu.VMEM((8, padded), F32),
        pltpu.VMEM((layers, 2, 8, 128), F32),
        pltpu.VMEM((ff, layers, features), BF16),
        pltpu.VMEM((ff, layers, features), BF16),
        pltpu.VMEM((layers, ff, features), BF16),
        pltpu.VMEM((layers, ff, features), BF16),
        pltpu.VMEM((layers, 128, features), BF16),
        pltpu.VMEM((3, rows, 128), F32),
        pltpu.VMEM((3, rows, 128), F32),
        pltpu.VMEM((ny, nj * nz, ff), BF16),
        pltpu.VMEM((nz, nj * ny, ff), BF16),
        pltpu.VMEM((ny, nj * nz, 128), F32),
        pltpu.VMEM((nz, nj * ny, 128), F32),
        buffers((layers, nz, 8), wide1),
        buffers((layers, nj, nz), data1),
        buffers((layers, ny, nj, nz), data1),
        buffers((ny, nj, nz), data1),
        buffers((layers, 2 * (ny - 1), hj, nz), data1),
        buffers((layers, 2 * (ny - 1), hj, nz), data1),
        buffers((layers, nj, nz), wide1),
        buffers((layers, nj, nz), wide1),
        buffers((layers, nz, 8), wide1),
        buffers((layers, nz, 8), wide1),
        buffers((layers, nz, ny, 8), wide2),
        buffers((layers, nz, nj, ny), data2),
        buffers((layers, nz, nj, ny), data2),
        buffers((nz, ny, 8), data2),
        buffers((layers, nz, nj, ny), data2),
        buffers((layers, nz, nj, ny), data2),
        buffers((layers, 2 * (nz - 1), hy, 8), data2),
        buffers((layers, 2 * (nz - 1), hy, 8), data2),
        buffers((layers, ny, 8), data2),
        buffers((layers, ny, 8), data2),
        dma((2,)),
        dma((layers, 12, 2)),
        dma((layers, 2)),
        dma((layers, 2)),
        dma((layers, 2, 2, 2, ny // 2)),
        dma((layers, 2)),
        dma((layers, 2, 2, 2, nz // 2)),
        dma((layers, 2, nz)),
        dma((layers, 2, 2 * (ny - 1))),
        dma((layers, 2)),
        dma((layers, 2)),
        dma((layers, 2, nz)),
        dma((layers, 2, 2 * (nz - 1))),
        dma((layers, 2)),
    ]
    vmem = pl.BlockSpec(memory_space=pltpu.VMEM)
    hbm = pl.BlockSpec(memory_space=pl.ANY)
    return pl.pallas_call(
        functools.partial(kernel, dims),
        out_shape=jax.ShapeDtypeStruct(tokens.shape, BF16),
        in_specs=[vmem, vmem, vmem, vmem, hbm, hbm],
        out_specs=vmem,
        scratch_shapes=scratch,
        compiler_params=pltpu.CompilerParams(
            collective_id=0, has_side_effects=True, vmem_limit_bytes=66_000_000
        ),
    )(
        tokens,
        jnp.transpose(routes, (0, 2, 1)),
        placement,
        jnp.transpose(router_weight, (1, 0, 2)),
        jnp.transpose(up_weight, (1, 3, 0, 2)),
        jnp.transpose(down_weight, (1, 2, 0, 3)),
    )


def solution(mesh, plane=8):
    return jax.shard_map(
        functools.partial(per_device, plane),
        mesh=mesh,
        in_specs=(
            P(("dp", "expert"), None),
            P(None, ("dp", "expert"), None),
            P(),
            P(None, "expert", None, "dp"),
            P(None, "expert", "dp", None),
            P(None, "expert", None),
        ),
        out_specs=P(("dp", "expert"), None),
        check_vma=False,
    )
```

```python
import functools

import jax
import jax.numpy as jnp
from jax import lax
from jax.experimental import pallas as pl
from jax.experimental.pallas import tpu as pltpu
from jax.sharding import PartitionSpec as P

MESH = pl.DeviceIdType.MESH
F32, BF16 = jnp.float32, jnp.bfloat16
NT = (((1,), (1,)), ((), ()))


def flat(value):
    width = value.shape[-1]
    return value.astype(F32).reshape(-1, width).astype(BF16)


def flat32(value):
    return value.astype(F32).reshape(-1, value.shape[-1])


def hops(direction, half, n):
    return n // 2 if (direction == 1) == (half == 0) else n // 2 - 1


def kernel(
    dims,
    tokens,
    routes,
    placement,
    router,
    up,
    down,
    out,
    stream,
    hot,
    up_w,
    down_w,
    up_v,
    down_v,
    router_v,
    h1,
    h2,
    hid1,
    hid2,
    gate1,
    gate2,
    zin1,
    xo1,
    rows1,
    part1,
    rs1o,
    rs1i,
    xr1o,
    xr1i,
    zr1o,
    zr1i,
    toks2,
    xo2,
    rows2,
    comb2,
    xr2o,
    xr2i,
    rs2o,
    rs2i,
    yr2o,
    yr2i,
    weight_sem,
    send_sem,
    z1_sem,
    x1_sem,
    ring1_sem,
    y2_sem,
    ring2_sem,
    x2_sem,
    rs1_sem,
    xr1_sem,
    zr1_sem,
    xr2_sem,
    rs2_sem,
    yr2_sem,
):
    ny, nz, nj, layers, features, cuts1, cuts2, ff = dims
    hj, hy = nj // 2, ny // 2
    y = lax.axis_index("dp")
    e = lax.axis_index("expert")
    z, j = e // nj, e % nj
    lanes = 128

    def at_y(other):
        return (other, e)

    def at_z(other):
        return (y, other * nj + j)

    def at_j(other):
        return (y, z * nj + other)

    def turn(a, n):
        return lax.rem(a + 2 * n, n)

    barrier = pltpu.get_barrier_semaphore()
    for d in range(1, ny):
        pl.semaphore_signal(barrier, inc=1, device_id=at_y(turn(y + d, ny)), device_id_type=MESH)
    for d in range(1, nz):
        pl.semaphore_signal(barrier, inc=1, device_id=at_z(turn(z + d, nz)), device_id_type=MESH)
    for d in range(1, nj):
        pl.semaphore_signal(barrier, inc=1, device_id=at_j(turn(j + d, nj)), device_id_type=MESH)

    weights = [
        pltpu.make_async_copy(up.at[0], up_w, weight_sem.at[0]),
        pltpu.make_async_copy(down.at[0], down_w, weight_sem.at[1]),
    ]
    for copy in weights:
        copy.start()

    for layer in range(layers):
        picks = routes[layer]
        count = placement.shape[1]
        names = lax.broadcasted_iota(jnp.int32, (count, picks.shape[1]), 0)
        named = jnp.zeros((count, picks.shape[1]), F32)
        for k in range(picks.shape[0]):
            named = named + jnp.where(picks[k : k + 1, :] == names, 1.0, 0.0)
        slot_of = jnp.broadcast_to(placement[layer : layer + 1, :], (lanes, count))
        slots = lax.broadcasted_iota(jnp.int32, (lanes, count), 0)
        for which, shift in ((0, 0), (1, lanes // 2)):
            serves = jnp.where(slot_of + shift == slots, 1.0, 0.0).astype(BF16)
            hot[layer, which] = lax.dot_general(
                named.astype(BF16), serves, (((0,), (1,)), ((), ())), preferred_element_type=F32
            )
    for layer in range(layers):
        gate_row = jnp.broadcast_to(router[0].astype(F32)[layer : layer + 1, :], (lanes, features)).astype(BF16)
        router_v[layer, :, 0:features] = gate_row

    stream[...] = jnp.zeros_like(stream)
    stream[:, 0:features] = tokens[...].astype(F32)

    def picker(blocks, low):
        rows = nj * blocks
        tokens_in = blocks * 8
        return rows, tokens_in, low

    def pick_matrix(hots, blocks, low):
        rows, columns, low = picker(blocks, low)
        row = lax.broadcasted_iota(jnp.int32, (rows, lanes), 0)
        slot = lax.broadcasted_iota(jnp.int32, (rows, lanes), 1)
        wanted = jnp.where(slot == low + z * nj + row // blocks, 1.0, 0.0).astype(BF16)
        same = (
            lax.broadcasted_iota(jnp.int32, (rows, columns), 0) % blocks
            == lax.broadcasted_iota(jnp.int32, (rows, columns), 1) // 8
        )
        product = lax.dot_general(wanted, hots, NT, preferred_element_type=F32)
        return jnp.where(same, product, 0.0).astype(BF16)

    def place_matrix(hots, blocks, low):
        rows, columns, low = picker(blocks, low)
        row = lax.broadcasted_iota(jnp.int32, (rows, lanes), 0)
        slot = lax.broadcasted_iota(jnp.int32, (rows, lanes), 1)
        wanted = jnp.where(slot == low + z * nj + row // blocks, 1.0, 0.0).astype(BF16)
        same = (
            lax.broadcasted_iota(jnp.int32, (columns, rows), 1) % blocks
            == lax.broadcasted_iota(jnp.int32, (columns, rows), 0) // 8
        )
        product = lax.dot_general(hots, wanted, NT, preferred_element_type=F32)
        return jnp.where(same, product, 0.0).astype(BF16)

    def send(src, dst, sent, landed, device):
        pltpu.make_async_remote_copy(
            src_ref=src, dst_ref=dst, send_sem=sent, recv_sem=landed, device_id=device, device_id_type=MESH
        ).start()

    def wait_bytes(ref, sem):
        pltpu.make_async_copy(ref, ref, sem).wait()

    (S_Z1, S_X1, S_RING1, S_Y2, S_RING2, S_X2, S_RS1, S_XR1, S_ZR1, S_XR2, S_RS2, S_YR2) = range(12)

    parts = (0, 1)

    def layer_body(l, carry):
        sent = lambda which, part: send_sem.at[l, which, part]

        values = stream[...]
        mean = jnp.sum(values * values, axis=1, keepdims=True) * (1.0 / features)
        normed = values * lax.rsqrt(mean + 1e-05)
        for p in parts:
            low, high = cuts1[p]
            zin1[p][l, z, :, 0 : high - low] = normed[:, low:high].astype(BF16)
            if p == 0:
                zin1[p][l, z, :, high - low : high - low + lanes] = hot[l, 0].astype(BF16)
            low, high = cuts2[p]
            if p == 0:
                full = (high - low) // lanes * lanes
                toks2[p][l, z, y, :, 0:full] = normed[:, low : low + full].astype(BF16)
                toks2[p][l, z, y, :, full : full + lanes] = (normed[:, low + full :] + hot[l, 1]).astype(BF16)
            else:
                toks2[p][l, z, y] = normed[:, low:high].astype(BF16)

        @pl.when(l == 0)
        def _():
            pl.semaphore_wait(barrier, ny + nz + nj - 3)

        for p in parts:
            for d in range(1, ny):
                block = toks2[p].at[l, z, y]
                send(block, block, sent(S_Y2, p), y2_sem.at[l, p], at_y(turn(y + d, ny)))
            for d in range(1, nz):
                block = zin1[p].at[l, z]
                send(block, block, sent(S_Z1, p), z1_sem.at[l, p], at_z(turn(z + d, nz)))

        @pl.when(l == 0)
        def _():
            for copy in weights:
                copy.wait()
            up_v[0] = up_w[:, 0, :]
            down_v[0] = down_w[:, 0, :]

        def ring_half(direction, long):
            return 0 if (direction == 1) == long else 1

        def ring2_send(origin, direction, half, step, p):
            part = toks2[p].at[l, origin, half * hy : (half + 1) * hy]
            landed = ring2_sem.at[l, p, (direction + 1) // 2, half, step - 1]
            send(part, part, sent(S_RING2, p), landed, at_z(turn(z + direction, nz)))

        def ring1_send(origin, direction, half, step, p):
            part = rows1[p].at[l, origin, half * hj : (half + 1) * hj]
            landed = ring1_sem.at[l, p, (direction + 1) // 2, half, step - 1]
            send(part, part, sent(S_RING1, p), landed, at_y(turn(y + direction, ny)))

        def ring2_step(step, p, long):
            for direction in (1, -1):
                half = ring_half(direction, long)
                origin = turn(z - direction * step, nz)
                if hops(direction, half, nz) >= step:
                    part = toks2[p].at[l, origin, half * hy : (half + 1) * hy]
                    wait_bytes(part, ring2_sem.at[l, p, (direction + 1) // 2, half, step - 1])
                    if hops(direction, half, nz) > step:
                        ring2_send(origin, direction, half, step + 1, p)

        def ring1_step(step, p, long):
            for direction in (1, -1):
                half = ring_half(direction, long)
                origin = turn(y - direction * step, ny)
                if hops(direction, half, ny) >= step:
                    part = rows1[p].at[l, origin, half * hj : (half + 1) * hj]
                    wait_bytes(part, ring1_sem.at[l, p, (direction + 1) // 2, half, step - 1])
                    if hops(direction, half, ny) > step:
                        ring1_send(origin, direction, half, step + 1, p)

        def start_ring(send_one, me, n, p):
            for long in (True, False):
                for direction in (1, -1):
                    half = ring_half(direction, long)
                    if hops(direction, half, n) >= 1:
                        send_one(me, direction, half, 1, p)

        def at_distance(me, d, n):
            return [turn(me + d, n)] if d == 0 or 2 * d == n else [turn(me + d, n), turn(me - d, n)]

        kept = {}

        def hots2(zc):
            width = cuts2[0][1] - cuts2[0][0]
            full = width // lanes * lanes
            return flat(toks2[0][l, zc, :, :, full : full + lanes])

        def exchange2(distance, p):
            for at, zc in enumerate(at_distance(z, distance, nz)):
                if p == 0:
                    kept["pick", distance, at] = pick_matrix(hots2(zc), ny, lanes // 2)
                width = cuts2[p][1] - cuts2[p][0]
                tokens_in = flat(toks2[p][l, zc, :, :, 0:width])
                rows = jnp.dot(kept["pick", distance, at], tokens_in, preferred_element_type=F32)
                xo2[p][l, zc] = rows.reshape(nj, ny, width).astype(BF16)
                rows2[p][l, zc, j] = xo2[p][l, zc, j]
                for d in range(1, nj):
                    other = turn(j + d, nj)
                    send(xo2[p].at[l, zc, other], rows2[p].at[l, zc, j], sent(S_X2, p), x2_sem.at[l, p, zc], at_j(other))

        def products(rows, cuts):
            hidden, gate = 0.0, 0.0
            for p in parts:
                low, high = cuts[p]
                hidden += lax.dot_general(rows[p], up_v[l, :, low:high], NT, preferred_element_type=F32)
                gate += lax.dot_general(rows[p], router_v[l, :, low:high], NT, preferred_element_type=F32)
            return hidden[:, 0:lanes], hidden[:, lanes:ff], gate

        def up1(yc):
            at = pl.ds(yc * (nj * nz), nj * nz)
            first, second, gate = products([flat(rows1[p][l, yc]) for p in parts], cuts1)
            h1[0, at, :] = first
            h1[1, at, 0 : ff - lanes] = second
            h1[2, at, :] = gate

        def up2(zc):
            for p in parts:
                wait_bytes(rows2[p].at[l, zc, 0 : nj - 1], x2_sem.at[l, p, zc])
            at = pl.ds(zc * (nj * ny), nj * ny)
            first, second, gate = products([flat(rows2[p][l, zc]) for p in parts], cuts2)
            h2[0, at, :] = first
            h2[1, at, 0 : ff - lanes] = second
            h2[2, at, :] = gate

        hots1 = None
        for p in parts:
            wait_bytes(toks2[p].at[l, 0, 0 : ny - 1], y2_sem.at[l, p])
            start_ring(ring2_send, z, nz, p)
            wait_bytes(zin1[p].at[l, 0 : nz - 1], z1_sem.at[l, p])
            width = cuts1[p][1] - cuts1[p][0]
            if p == 0:
                hots1 = flat(zin1[p][l, :, :, width : width + lanes])
                pick1 = pick_matrix(hots1, nz, 0)
            picked = jnp.dot(pick1, flat(zin1[p][l, :, :, 0:width]), preferred_element_type=F32)
            xo1[p][l] = picked.reshape(nj, nz, width).astype(BF16)
            rows1[p][l, y, j] = xo1[p][l, j]
            for d in range(1, nj):
                other = turn(j + d, nj)
                send(xo1[p].at[l, other], rows1[p].at[l, y, j], sent(S_X1, p), x1_sem.at[l, p], at_j(other))
        for p in parts:
            exchange2(0, p)

        steps2, steps1 = nz // 2, ny // 2
        for step in range(1, max(steps2, steps1 + 1) + 1):
            behind = step - 1
            for p in parts:
                if step <= steps2:
                    ring2_step(step, p, True)
                if step == 1:
                    wait_bytes(rows1[p].at[l, y, 0 : nj - 1], x1_sem.at[l, p])
                    start_ring(ring1_send, y, ny, p)
                elif behind <= steps1:
                    ring1_step(behind, p, True)
                if step <= steps2:
                    ring2_step(step, p, False)
                    exchange2(step, p)
                if 1 <= behind <= steps1:
                    ring1_step(behind, p, False)
            if behind <= steps1:
                for yc in at_distance(y, behind, ny):
                    up1(yc)
            if behind <= steps2:
                for zc in at_distance(z, behind, nz):
                    up2(zc)
        for behind in range(max(steps2, steps1 + 1), steps2 + 1):
            for zc in at_distance(z, behind, nz):
                up2(zc)

        def silu(v):
            return v / (1.0 + jnp.exp(-v))

        def sigmoid(v):
            return 1.0 / (1.0 + jnp.exp(-v))

        def join(chunk, own, other, ours, theirs, hidden, gate):
            base = pl.multiple_of(chunk * (nj * theirs), nj * theirs)
            total = []
            for lane in range(3):
                tiles = [other[lane, pl.ds(jc * ours + chunk, theirs, stride=nj * ours), :] for jc in range(nj)]
                total.append(own[lane, pl.ds(base, nj * theirs), :] + jnp.concatenate(tiles, axis=0))
            hidden[chunk, :, 0:lanes] = silu(total[0]).astype(BF16)
            hidden[chunk, :, lanes:ff] = silu(total[1])[:, 0 : ff - lanes].astype(BF16)
            gate[chunk] = sigmoid(total[2]).astype(BF16).astype(F32)

        def down2(distance):
            for zc in at_distance(z, distance, nz):
                join(zc, h2, h1, nz, ny, hid2, gate2)
                for p in parts:
                    low, high = cuts2[p]
                    result = jnp.dot(hid2[zc], down_v[l, :, low:high], preferred_element_type=F32)
                    result = result * gate2[zc][:, 0:1]
                    xr2o[p][l, zc] = result.reshape(nj, ny, high - low).astype(BF16)
                    xr2i[p][l, zc, j] = xr2o[p][l, zc, j]
                    for d in range(1, nj):
                        other = turn(j + d, nj)
                        send(
                            xr2o[p].at[l, zc, other], xr2i[p].at[l, zc, j], sent(S_XR2, p), xr2_sem.at[l, p, zc], at_j(other)
                        )

        def down1(distance):
            if ("part", distance) in kept or distance < 0:
                return
            kept["part", distance] = True
            for yc in at_distance(y, distance, ny):
                join(yc, h1, h2, ny, nz, hid1, gate1)
                for p in parts:
                    low, high = cuts1[p]
                    result = jnp.dot(hid1[yc], down_v[l, :, low:high], preferred_element_type=F32)
                    result = result * gate1[yc][:, 0:1]
                    part1[p][yc] = result.reshape(nj, nz, high - low).astype(BF16)

        def need2(distance, p):
            for at, zc in enumerate(at_distance(z, distance, nz)):
                if ("sum", distance, at, p) in kept:
                    continue
                kept["sum", distance, at, p] = True
                if p == 0:
                    kept["place", distance, at] = place_matrix(hots2(zc), ny, lanes // 2)
                wait_bytes(xr2i[p].at[l, zc, 0 : nj - 1], xr2_sem.at[l, p, zc])
                total = jnp.dot(kept["place", distance, at], flat(xr2i[p][l, zc]), preferred_element_type=F32)
                comb2[p][zc] = total.reshape(ny, 8, total.shape[1]).astype(BF16)

        def slot_of_send(moving, half, step, n):
            order = []
            for m in (1, -1):
                for h in (0, 1):
                    for s in range(1, hops(-m, h, n) + 1):
                        order.append((m, h, s))
            return order.index((moving, half, step))

        def reduce_step(me, n, size, own, outgoing, incoming, sems, sent_sem, to, step, long):
            for moving in (1, -1):
                half = ring_half(-moving, long)
                length = hops(-moving, half, n)
                if length < step:
                    continue
                dest = turn(me + moving * (length + 1 - step), n)
                value = own[dest, half * size : (half + 1) * size]
                slot = slot_of_send(moving, half, step, n)
                if step > 1:
                    before = slot_of_send(moving, half, step - 1, n)
                    wait_bytes(incoming.at[l, before], sems(before))
                    value = (value.astype(F32) + incoming[l, before].astype(F32)).astype(BF16)
                outgoing[l, slot] = value
                send(outgoing.at[l, slot], incoming.at[l, slot], sent_sem, sems(slot), to(turn(me + moving, n)))

        def reduce_end(me, n, size, own, incoming, sems):
            halves = []
            for half in (0, 1):
                total = own[me, half * size : (half + 1) * size].astype(F32)
                for moving in (1, -1):
                    length = hops(-moving, half, n)
                    if length >= 1:
                        slot = slot_of_send(moving, half, length, n)
                        wait_bytes(incoming.at[l, slot], sems(slot))
                        total = total + incoming[l, slot].astype(F32)
                halves.append(total)
            return halves

        def reduce1(step, p, long):
            reduce_step(
                y, ny, hj, part1[p], rs1o[p], rs1i[p], lambda slot: rs1_sem.at[l, p, slot], sent(S_RS1, p), at_y, step, long
            )

        def reduce2(step, p, long):
            reduce_step(
                z, nz, hy, comb2[p], rs2o[p], rs2i[p], lambda slot: rs2_sem.at[l, p, slot], sent(S_RS2, p), at_z, step, long
            )

        def finish1(p):
            width = cuts1[p][1] - cuts1[p][0]
            ended = reduce_end(y, ny, hj, part1[p], rs1i[p], lambda slot: rs1_sem.at[l, p, slot])
            for half, total in enumerate(ended):
                xr1o[p][l, half * hj : (half + 1) * hj, :, 0:width] = total.astype(BF16)
            if p == 0:
                xr1o[p][l, :, :, width : width + lanes] = gate1[y].reshape(nj, nz, lanes).astype(BF16)
            xr1i[p][l, j] = xr1o[p][l, j]
            for d in range(1, nj):
                other = turn(j + d, nj)
                send(xr1o[p].at[l, other], xr1i[p].at[l, j], sent(S_XR1, p), xr1_sem.at[l, p], at_j(other))

        for d in range(steps2, steps2 - 2, -1):
            down2(d)
            down1(steps1 - steps2 + d)
            for p in parts:
                reduce1(1, p, d == steps2)
        for d in range(steps2 - 2, -1, -1):
            down2(d)
        for step in range(1, max(steps1, steps2) + 1):
            for long in (True, False):
                if step == max(steps1 - 1, 1):
                    down1(0)
                down1(steps1 - step if long else steps1 - 1 - step)
                for p in parts:
                    reduce1(step + 1, p, long)
                    distance = steps2 + 1 - step if long else steps2 - step
                    if distance >= 1:
                        need2(distance, p)
                        reduce2(step, p, long)
                if step == (max(steps1 - 1, 1) if not long else steps1) and steps1 > 1:
                    finish1(1 if long else 0)
        if steps1 == 1:
            finish1(0)
            finish1(1)
        for p in parts:
            need2(0, p)

        place1 = place_matrix(flat(zin1[0][l, :, :, cuts1[0][1] : cuts1[0][1] + lanes]), nz, 0)
        for p in parts:
            width = cuts1[p][1] - cuts1[p][0]
            wait_bytes(xr1i[p].at[l, 0 : nj - 1], xr1_sem.at[l, p])
            sums = jnp.dot(place1, flat(xr1i[p][l]), preferred_element_type=F32)
            zr1o[p][l, :, :, 0:width] = sums[:, 0:width].reshape(nz, 8, width).astype(BF16)
            if p == 0:
                gates = sums[:, width:]
                rounded = gates.astype(BF16).astype(F32)
                lane = lax.broadcasted_iota(jnp.int32, gates.shape, 1)
                pair = jnp.where(lane < lanes // 2, rounded, gates - rounded)
                zr1o[p][l, :, :, width : width + lanes] = pair.reshape(nz, 8, lanes).astype(BF16)
            zr1i[p][l, z] = zr1o[p][l, z]
            for d in range(1, nz):
                other = turn(z + d, nz)
                send(zr1o[p].at[l, other], zr1i[p].at[l, z], sent(S_ZR1, p), zr1_sem.at[l, p], at_z(other))

            ended = reduce_end(z, nz, hy, comb2[p], rs2i[p], lambda slot: rs2_sem.at[l, p, slot])
            for half, total in enumerate(ended):
                yr2o[p][l, half * hy : (half + 1) * hy] = total.astype(BF16)
            yr2i[p][l, y] = yr2o[p][l, y]
            for d in range(1, ny):
                other = turn(y + d, ny)
                send(yr2o[p].at[l, other], yr2i[p].at[l, y], sent(S_YR2, p), yr2_sem.at[l, p], at_y(other))

        @pl.when(l == 0)
        def _():
            for layer in range(1, layers):
                up_v[layer] = up_w[:, layer, :]
                down_v[layer] = down_w[:, layer, :]

        denom = None
        for p in parts:
            low, high = cuts1[p]
            wait_bytes(zr1i[p].at[l, 0 : nz - 1], zr1_sem.at[l, p])
            both = jnp.sum(zr1i[p][l].astype(F32), axis=0)
            if p == 0:
                width = high - low
                denom = both[:, width : width + 1] + both[:, width + lanes // 2 : width + lanes // 2 + 1]
                denom = jnp.maximum(denom, 0.5)
            stream[:, low:high] = (stream[:, low:high] + both[:, 0 : high - low] / denom).astype(BF16).astype(F32)
            low, high = cuts2[p]
            wait_bytes(yr2i[p].at[l, 0 : ny - 1], yr2_sem.at[l, p])
            numer = jnp.sum(yr2i[p][l].astype(F32), axis=0)
            stream[:, low:high] = (stream[:, low:high] + numer / denom).astype(BF16).astype(F32)

        for p in parts:
            wait_bytes(zin1[p].at[l, 0 : nz - 1], sent(S_Z1, p))
            wait_bytes(xo1[p].at[l, 0 : nj - 1], sent(S_X1, p))
            wait_bytes(rows1[p].at[l, 0 : ny - 1], sent(S_RING1, p))
            wait_bytes(toks2[p].at[l, 0, 0 : ny - 1], sent(S_Y2, p))
            wait_bytes(toks2[p].at[l, 0 : nz - 1], sent(S_RING2, p))
            wait_bytes(xo2[p].at[l, :, 0 : nj - 1], sent(S_X2, p))
            wait_bytes(rs1o[p].at[l], sent(S_RS1, p))
            wait_bytes(xr1o[p].at[l, 0 : nj - 1], sent(S_XR1, p))
            wait_bytes(zr1o[p].at[l, 0 : nz - 1], sent(S_ZR1, p))
            wait_bytes(xr2o[p].at[l, :, 0 : nj - 1], sent(S_XR2, p))
            wait_bytes(rs2o[p].at[l], sent(S_RS2, p))
            wait_bytes(yr2o[p].at[l, 0 : ny - 1], sent(S_YR2, p))
        return carry

    lax.fori_loop(0, layers, layer_body, 0)
    out[...] = stream[:, 0:features].astype(BF16)


def per_device(plane, tokens, routes, placement, up_weight, down_weight, router_weight):
    ny = lax.axis_size("dp")
    nj = plane
    nz = lax.axis_size("expert") // nj
    layers, _, features, ff = up_weight.shape
    tiles = features // 128
    tiles1 = tiles // 2 + (1 if tiles > 8 else 0)
    first1 = tiles1 // 2 * 128
    w1 = tiles1 * 128
    second2 = w1 + (tiles - tiles1) // 2 * 128
    cuts1 = ((0, first1), (first1, w1))
    cuts2 = ((second2, features), (w1, second2))
    padded = -(-features // 128) * 128
    hj, hy = nj // 2, ny // 2
    dims = (ny, nz, nj, layers, features, cuts1, cuts2, ff)
    rows = ny * nz * nj
    dma = pltpu.SemaphoreType.DMA
    data1 = [high - low for low, high in cuts1]
    wide1 = [data1[0] + 128, data1[1]]
    data2 = [high - low for low, high in cuts2]
    wide2 = [padded - second2, data2[1]]

    def buffers(shape, widths):
        return [pltpu.VMEM((*shape, width), BF16) for width in widths]

    scratch = [
        pltpu.VMEM((8, padded), F32),
        pltpu.VMEM((layers, 2, 8, 128), F32),
        pltpu.VMEM((ff, layers, features), BF16),
        pltpu.VMEM((ff, layers, features), BF16),
        pltpu.VMEM((layers, ff, features), BF16),
        pltpu.VMEM((layers, ff, features), BF16),
        pltpu.VMEM((layers, 128, features), BF16),
        pltpu.VMEM((3, rows, 128), F32),
        pltpu.VMEM((3, rows, 128), F32),
        pltpu.VMEM((ny, nj * nz, ff), BF16),
        pltpu.VMEM((nz, nj * ny, ff), BF16),
        pltpu.VMEM((ny, nj * nz, 128), F32),
        pltpu.VMEM((nz, nj * ny, 128), F32),
        buffers((layers, nz, 8), wide1),
        buffers((layers, nj, nz), data1),
        buffers((layers, ny, nj, nz), data1),
        buffers((ny, nj, nz), data1),
        buffers((layers, 2 * (ny - 1), hj, nz), data1),
        buffers((layers, 2 * (ny - 1), hj, nz), data1),
        buffers((layers, nj, nz), wide1),
        buffers((layers, nj, nz), wide1),
        buffers((layers, nz, 8), wide1),
        buffers((layers, nz, 8), wide1),
        buffers((layers, nz, ny, 8), wide2),
        buffers((layers, nz, nj, ny), data2),
        buffers((layers, nz, nj, ny), data2),
        buffers((nz, ny, 8), data2),
        buffers((layers, nz, nj, ny), data2),
        buffers((layers, nz, nj, ny), data2),
        buffers((layers, 2 * (nz - 1), hy, 8), data2),
        buffers((layers, 2 * (nz - 1), hy, 8), data2),
        buffers((layers, ny, 8), data2),
        buffers((layers, ny, 8), data2),
        dma((2,)),
        dma((layers, 12, 2)),
        dma((layers, 2)),
        dma((layers, 2)),
        dma((layers, 2, 2, 2, ny // 2)),
        dma((layers, 2)),
        dma((layers, 2, 2, 2, nz // 2)),
        dma((layers, 2, nz)),
        dma((layers, 2, 2 * (ny - 1))),
        dma((layers, 2)),
        dma((layers, 2)),
        dma((layers, 2, nz)),
        dma((layers, 2, 2 * (nz - 1))),
        dma((layers, 2)),
    ]
    vmem = pl.BlockSpec(memory_space=pltpu.VMEM)
    hbm = pl.BlockSpec(memory_space=pl.ANY)
    return pl.pallas_call(
        functools.partial(kernel, dims),
        out_shape=jax.ShapeDtypeStruct(tokens.shape, BF16),
        in_specs=[vmem, vmem, vmem, vmem, hbm, hbm],
        out_specs=vmem,
        scratch_shapes=scratch,
        compiler_params=pltpu.CompilerParams(
            collective_id=0, has_side_effects=True, vmem_limit_bytes=66_000_000
        ),
    )(
        tokens,
        jnp.transpose(routes, (0, 2, 1)),
        placement,
        jnp.transpose(router_weight, (1, 0, 2)),
        jnp.transpose(up_weight, (1, 3, 0, 2)),
        jnp.transpose(down_weight, (1, 2, 0, 3)),
    )


def solution(mesh, plane=8):
    return jax.shard_map(
        functools.partial(per_device, plane),
        mesh=mesh,
        in_specs=(
            P(("dp", "expert"), None),
            P(None, ("dp", "expert"), None),
            P(),
            P(None, "expert", None, "dp"),
            P(None, "expert", "dp", None),
            P(None, "expert", None),
        ),
        out_specs=P(("dp", "expert"), None),
        check_vma=False,
    )
```
